256 devices in a mesh: pair: 32 (over y, x, core), sec: 8 (over z).
Axes of the slice: x: 4, y: 4, z: 8, core: 2. Of those that a mesh axis runs over, the one named last changes fastest.
Arguments:
- source: float32 [16384, 4096], P('sec', 'pair'), may hold values from -6 to 6
- occ_energy: float32 [4096], P('pair'), may hold values from 0.5 to 2
- virt_energy: float32 [16384], P('sec'), may hold values from 0.5 to 2
- v_tiles: float32 [256, 256, 256], P('sec'), may hold values from -0.12 to 0.12
- v_rows: int32 [256], P('sec'), may hold values from 0 to 11, as said below
- v_cols: int32 [256], P('sec'), may hold values from 0 to 7
- v_count: int32 [8], P('sec'), may hold values from 8 to 32, as said below
- w_tiles: float32 [48, 128, 128], replicated, may hold values from -0.18 to 0.18
- w_rows: int32 [48], replicated, may hold values from 0 to 31, as said below
- w_cols: int32 [48], replicated, may hold values from 0 to 31, as said below
Outputs:
- amplitudes: float32 [16384, 4096], P('sec', 'pair')
The draws below stay inside these ranges and needn't reach their ends.
Inputs may be any that keep to these rules, and one draw needn't show every extreme that they name: Entry n belongs to section s = n // 32; its row tile s * 8 - 2 + v_rows[n] lies inside the virtual range and differs from its column tile by at most 2. In every section but the first some used entry has v_rows 0 and some has 1; in every section but the last some used entry has 10 and some has 11. Only the first v_count[s] entries of section s are used; one section uses all 32, every other one at most 16. `w_rows`: every tile index appears; a pair may repeat, and repeated tiles add. `w_cols`: every tile index appears.
All inputs are finite; a program needn't handle non-finite values.
Results may differ from the reference program's by a relative error of at most 0.0003.
Values sent between devices are 32-bit elements; how exact they have to be, the bound alone decides.
A program may use at most 128 MiB of HBM per device.

```python
import math
import jax
import jax.numpy as jnp
from jax import lax

OCC = 4096
VIRT = 16384
VT = 256
OT = 128
VSLOTS = 32
WSLOTS = 48
ITERS = 3
TSEC = 8
NT = 32
N_SEC = 8


def v_lists(key):
    key = jax.random.fold_in(key, 101)
    candidates = 5 * TSEC
    base = jnp.arange(candidates, dtype=jnp.int32)
    column = base // 5
    offset = base % 5 - 2
    section_keys = jax.random.split(key, N_SEC + 2)

    def one_section(section_key, section):
        global_row = section * TSEC + column + offset
        valid = ((global_row >= 0) & (global_row < TSEC * N_SEC)).astype(jnp.int32)
        lower = ((column == 0) | (column == 1)) & (offset == -2)
        upper = ((column == TSEC - 1) | (column == TSEC - 2)) & (offset == 2)
        forced = (lower | upper).astype(jnp.int32)
        score = jax.random.permutation(section_key, candidates).astype(jnp.int32) + 1000 * forced - 100000 * (1 - valid)
        chosen = lax.top_k(score, VSLOTS)[1]
        return (column[chosen] + offset[chosen] + 2, column[chosen])
    rows_all, cols_all = jax.vmap(one_section)(section_keys[:N_SEC], jnp.arange(N_SEC, dtype=jnp.int32))
    busiest = jax.random.randint(section_keys[N_SEC], (), 0, N_SEC)
    lowest = max(VSLOTS // 4, 4)
    highest = max(VSLOTS // 2, lowest)
    counts = jax.random.randint(section_keys[N_SEC + 1], (N_SEC,), lowest, highest + 1)
    counts = jnp.where(jnp.arange(N_SEC) == busiest, VSLOTS, counts)
    return (rows_all.reshape(-1).astype(jnp.int32), cols_all.reshape(-1).astype(jnp.int32), counts.astype(jnp.int32))


def draw_v_rows(key, part):
    return v_lists(key)[0]


def draw_v_cols(key, part):
    return v_lists(key)[1]


def draw_v_count(key, part):
    return v_lists(key)[2]


def w_lists(key):
    key = jax.random.fold_in(key, 202)
    keys = jax.random.split(key, 4)
    extra = WSLOTS - NT
    rows_all = jnp.concatenate([jax.random.permutation(keys[0], NT).astype(jnp.int32), jax.random.randint(keys[2], (extra,), 0, NT).astype(jnp.int32)])
    cols_all = jnp.concatenate([jax.random.permutation(keys[1], NT).astype(jnp.int32), jax.random.randint(keys[3], (extra,), 0, NT).astype(jnp.int32)])
    return (rows_all, cols_all)


def draw_w_rows(key, part):
    return w_lists(key)[0]


def draw_w_cols(key, part):
    return w_lists(key)[1]


def levels(stream_key, extent, cuts, low, high):
    def one(dim, parts):
        draws = jax.random.uniform(jax.random.fold_in(jax.random.fold_in(stream_key, 6), dim), (parts,), jnp.float32, low / len(cuts), high / len(cuts))
        return jnp.repeat(jnp.exp(draws), extent[dim] // parts).reshape((-1,) + (1,) * (len(extent) - dim - 1))

    factor_of = one(*cuts[0])
    for cut in cuts[1:]:
        factor_of = factor_of * one(*cut)
    return factor_of


def noise(own_key, shape, spread, bound, pieces=(), kind=jnp.bfloat16):
    drawn = spread * jax.random.normal(own_key, shape, jnp.float32)
    if pieces:
        drawn = drawn * levels(own_key, shape, pieces, -0.22, 0.18)
    return jnp.clip(drawn, -bound, bound).astype(kind)


def setup_inputs(seed: int = 0) -> dict:
    key_of = jax.random.split(jax.random.key(seed), 11)
    return {
        "source": noise(key_of[0], (VIRT, OCC), 1.0, 6.0, ((0, 8), (1, 32)), jnp.float32),
        "occ_energy": jnp.clip(jnp.exp(math.log(2.0) - 1.3862944 * jax.random.uniform(key_of[1], (OCC,), jnp.float32) ** levels(key_of[1], (OCC,), ((0, 32),), -0.2, 0.2)), 0.5, 2.0),
        "virt_energy": jnp.clip(jnp.exp(math.log(2.0) - 1.3862944 * jax.random.uniform(key_of[2], (VIRT,), jnp.float32) ** levels(key_of[2], (VIRT,), ((0, 8),), -0.2, 0.2)), 0.5, 2.0),
        "v_tiles": noise(key_of[3], (N_SEC * VSLOTS, VT, VT), 0.02, 0.12, ((0, 8),), jnp.float32),
        "v_rows": draw_v_rows(jax.random.fold_in(key_of[10], 71), 0),
        "v_cols": draw_v_cols(jax.random.fold_in(key_of[10], 71), 0),
        "v_count": draw_v_count(jax.random.fold_in(key_of[10], 71), 0),
        "w_tiles": noise(key_of[7], (WSLOTS, OT, OT), 0.03, 0.18, (), jnp.float32),
        "w_rows": draw_w_rows(jax.random.fold_in(key_of[10], 71), 0),
        "w_cols": draw_w_cols(jax.random.fold_in(key_of[10], 71), 0),
    }


def hole_local(amplitude, w_tiles, w_rows, w_cols):
    local_rows = amplitude.shape[0]
    tile_order = w_tiles.shape[1]
    count_tiles = amplitude.shape[1] // tile_order
    blocked = amplitude.reshape(local_rows, count_tiles, tile_order)
    picked = jnp.take(blocked, w_cols, axis=1)
    contrib = jnp.einsum("lsv,suv->lsu", picked, w_tiles, precision=lax.Precision.HIGHEST)
    selector = (w_rows[:, None] == jnp.arange(count_tiles, dtype=jnp.int32)[None, :]).astype(jnp.float32)
    placed = jnp.einsum("lsu,si->liu", contrib, selector, precision=lax.Precision.HIGHEST)
    return placed.reshape(local_rows, count_tiles * tile_order)


def particle_ref(amplitude, v_tiles, v_rows, v_cols, v_count):
    tile_order = v_tiles.shape[1]
    padded = jnp.pad(amplitude, ((2 * tile_order, 2 * tile_order), (0, 0)))

    def add_tile(position, running):
        section = (position // VSLOTS).astype(jnp.int32)
        offset = (position % VSLOTS).astype(jnp.int32)

        def apply_tile(inner):
            one_tile = lax.dynamic_index_in_dim(v_tiles, position, 0, keepdims=False)
            row_start = ((section * TSEC + v_rows[position]) * tile_order).astype(jnp.int32)
            slab = lax.dynamic_slice_in_dim(padded, row_start, tile_order, 0)
            product = lax.dot_general(one_tile, slab, (((0,), (0,)), ((), ())), precision=lax.Precision.HIGHEST, preferred_element_type=jnp.float32)
            col_start = ((section * TSEC + v_cols[position]) * tile_order).astype(jnp.int32)
            current = lax.dynamic_slice_in_dim(inner, col_start, tile_order, 0)
            return lax.dynamic_update_slice_in_dim(inner, current + product, col_start, 0)

        def keep_total(inner):
            return inner

        return lax.cond(offset < v_count[section], apply_tile, keep_total, running)

    return lax.fori_loop(jnp.int32(0), jnp.int32(N_SEC * VSLOTS), add_tile, jnp.zeros_like(amplitude))


def hole_ref(amplitude, w_tiles, w_rows, w_cols):
    block_rows = min(1024, VIRT)
    stacked = amplitude.reshape(VIRT // block_rows, block_rows, OCC)

    def inner(piece):
        return hole_local(piece, w_tiles, w_rows, w_cols)

    return lax.map(inner, stacked).reshape(VIRT, OCC)


def reference(source, occ_energy, virt_energy, v_tiles, v_rows, v_cols, v_count, w_tiles, w_rows, w_cols):
    denom = virt_energy[:, None] + occ_energy[None, :]
    current = source / denom
    for iteration in range(ITERS):
        ladder_p = particle_ref(current, v_tiles, v_rows, v_cols, v_count)
        ladder_h = hole_ref(current, w_tiles, w_rows, w_cols)
        current = (source + ladder_p + ladder_h) / denom
    return current
```

```python
import functools

import jax
import jax.numpy as jnp
from jax import lax
from jax.experimental import pallas as pl
from jax.experimental.pallas import tpu as pltpu
from jax.sharding import PartitionSpec as P

MESH = pl.DeviceIdType.MESH
VT = 256
OT = 128
REACH = 2
SPAN = 2 * REACH + 1
F32 = jnp.float32
BF16 = jnp.bfloat16


def split(x):
    high = x.astype(BF16)
    low = (x - high.astype(F32)).astype(BF16)
    return high, low


def tables_kernel(v_rows, v_cols, v_count, w_rows, last_v, prev_v, last_w, prev_w):
    slots, section = v_rows.shape[0], last_v.shape[0] // SPAN
    wslots, tiles = w_rows.shape[0], last_w.shape[0]

    @pl.loop(0, section * SPAN)
    def _(i):
        last_v[i] = slots

    @pl.loop(0, tiles)
    def _(i):
        last_w[i] = wslots

    @pl.loop(0, slots)
    def _(n):
        prev_v[n] = slots

    @pl.loop(0, v_count[0])
    def _(n):
        key = v_cols[n] * SPAN + v_rows[n] - v_cols[n]
        prev_v[n] = last_v[key]
        last_v[key] = n

    @pl.loop(0, wslots)
    def _(n):
        key = w_rows[n]
        prev_w[n] = last_w[key]
        last_w[key] = n


def tables(v_rows, v_cols, v_count, w_rows, section, tiles):
    smem = pl.BlockSpec(memory_space=pltpu.SMEM)
    i32 = lambda n: jax.ShapeDtypeStruct((n,), jnp.int32)
    return pl.pallas_call(
        tables_kernel,
        out_shape=(i32(section * SPAN), i32(v_rows.shape[0]), i32(tiles), i32(w_rows.shape[0])),
        in_specs=[smem] * 4,
        out_specs=(smem,) * 4,
        name="tables",
    )(v_rows, v_cols, v_count, w_rows)


def far_first():
    steps = [(dx, dy, dc) for dx in range(-1, 3) for dy in range(-1, 3) for dc in range(2)]
    steps.remove((0, 0, 0))
    return sorted(steps, key=lambda s: -abs(s[0]) - abs(s[1]))


def partners(me, count):
    if count != 32:
        return [lax.rem(me + k, count) for k in range(1, count)]
    y, x, c = lax.div(me, 8), lax.rem(lax.div(me, 2), 4), lax.rem(me, 2)
    return [
        lax.rem(y + dy + 4, 4) * 8 + lax.rem(x + dx + 4, 4) * 2 + lax.rem(c + dc, 2)
        for dx, dy, dc in far_first()
    ]


def kernel(
    count,
    sections,
    last_v,
    prev_v,
    last_w,
    prev_w,
    w_cols,
    source,
    occ,
    virt,
    v_tiles,
    w_tiles,
    out,
    s_buf,
    occ_own,
    occ_all,
    virt_rows,
    virt_wide,
    v_stage,
    w_stage,
    v_split,
    w_split,
    start_a,
    scale_a,
    start_b,
    scale_b,
    part_a,
    part_b,
    hole_b,
    hole_a,
    window,
    split_b,
    chain,
    edge,
    halo,
    load_sem,
    v_sem,
    occ_sem,
    send_sem,
    recv_sem,
    edge_sem,
    halo_sem,
):
    rows = source.shape[0]
    block = rows // count
    section = rows // VT
    slots = v_tiles.shape[0] // VT
    wslots = w_tiles.shape[0] // OT
    groups = v_sem.shape[0]
    per_group = slots // groups
    me = lax.axis_index("pair")
    z = lax.axis_index("sec")
    up, down = lax.rem(z + 1, sections), lax.rem(z + sections - 1, sections)

    loads = [
        pltpu.make_async_copy(source, s_buf, load_sem.at[0]),
        pltpu.make_async_copy(occ, occ_own, load_sem.at[1]),
        pltpu.make_async_copy(virt, virt_rows, load_sem.at[2]),
    ]
    for copy in loads:
        copy.start()
    v_loads = []
    for g in range(groups):
        part = pl.ds(g * per_group * VT, per_group * VT)
        v_loads.append(pltpu.make_async_copy(v_tiles.at[part], v_stage.at[part], v_sem.at[g]))
        v_loads[-1].start()
    w_load = pltpu.make_async_copy(w_tiles, w_stage, load_sem.at[3])
    w_load.start()

    barrier = pltpu.get_barrier_semaphore()

    @pl.loop(1, count)
    def _(k):
        pl.semaphore_signal(
            barrier, inc=1, device_id={"pair": lax.rem(me + k, count)}, device_id_type=MESH
        )

    pl.semaphore_signal(barrier, inc=1, device_id={"sec": up}, device_id_type=MESH)
    pl.semaphore_signal(barrier, inc=1, device_id={"sec": down}, device_id_type=MESH)

    v_split[slots] = jnp.zeros((2, VT, VT), BF16)
    chain[wslots] = jnp.zeros((block, OT), F32)

    def blk(d):
        return pl.ds(pl.multiple_of(d * block, block), block)

    own = blk(me)
    others = partners(me, count)

    for copy in loads:
        copy.wait()

    def wide(row):
        return jnp.transpose(jnp.broadcast_to(row, (128, 128)))

    @pl.loop(0, rows // 128)
    def _(j):
        at = pl.ds(pl.multiple_of(j * 128, 128), 128)
        scale = 1.0 / (wide(virt_rows[pl.ds(j, 1), :]) + occ_own[...])
        scale_a[at, :] = scale
        start_a[at, :] = s_buf[at, :] * scale

    pl.semaphore_wait(barrier, count - 1 + 2)

    edge_rows = REACH * VT

    def send_edges(k, ref):
        for side, (first, where) in enumerate(((0, down), (rows - edge_rows, up))):
            base = (1 - side) * edge_rows
            pltpu.make_async_remote_copy(
                src_ref=ref.at[pl.ds(first, edge_rows)],
                dst_ref=halo.at[k, pl.ds(base, edge_rows)],
                send_sem=edge_sem.at[k, side],
                recv_sem=halo_sem.at[k, side],
                device_id={"sec": where},
                device_id_type=MESH,
            ).start()

    def wait_edges(k, ref, what):
        for side, (first, where) in enumerate(((0, down), (rows - edge_rows, up))):
            base = (1 - side) * edge_rows
            copy = pltpu.make_async_remote_copy(
                src_ref=ref.at[pl.ds(first, edge_rows)],
                dst_ref=halo.at[k, pl.ds(base, edge_rows)],
                send_sem=edge_sem.at[k, side],
                recv_sem=halo_sem.at[k, side],
                device_id={"sec": where},
                device_id_type=MESH,
            )
            if what == "recv":
                copy.wait_recv()
            else:
                copy.wait_send()

    def send_blocks(phase, src, dst):
        for d in others:
            pltpu.make_async_remote_copy(
                src_ref=src.at[blk(d)],
                dst_ref=dst.at[own],
                send_sem=send_sem.at[phase],
                recv_sem=recv_sem.at[phase],
                device_id={"pair": d},
                device_id_type=MESH,
            ).start()

    def wait_blocks(phase, src, dst, what):
        all_but_one = pl.ds(0, rows - block)
        copy = pltpu.make_async_remote_copy(
            src_ref=src.at[all_but_one],
            dst_ref=dst.at[all_but_one],
            send_sem=send_sem.at[phase],
            recv_sem=recv_sem.at[phase],
            device_id={"pair": others[0]},
            device_id_type=MESH,
        )
        if what == "recv":
            copy.wait_recv()
        else:
            copy.wait_send()

    send_edges(0, start_a)
    for d in others:
        pltpu.make_async_remote_copy(
            src_ref=occ_own,
            dst_ref=occ_all.at[me],
            send_sem=occ_sem.at[0],
            recv_sem=occ_sem.at[1],
            device_id={"pair": d},
            device_id_type=MESH,
        ).start()
    send_blocks(0, start_a, start_b)
    occ_all[pl.ds(me, 1)] = occ_own[...].reshape(1, 1, 128)
    start_b[own, :] = start_a[own, :]

    def put_window(at, values):
        high, low = split(values)
        window[at, 0:128] = high
        window[at, 128:256] = low

    def put_halo(k):
        for side in range(2):
            for i in range(REACH):
                src = pl.ds(side * edge_rows + i * VT, VT)
                first = i * VT if side == 0 else (REACH + section + i) * VT
                put_window(pl.ds(first, VT), halo[k, src, :])

    @pl.loop(0, section)
    def _(i):
        put_window(
            pl.ds(pl.multiple_of((i + REACH) * VT, VT), VT),
            start_a[pl.ds(pl.multiple_of(i * VT, VT), VT), :],
        )

    for g in range(groups):
        v_loads[g].wait()

        @pl.loop(g * per_group, (g + 1) * per_group)
        def _(n):
            tile = jnp.transpose(v_stage[pl.ds(pl.multiple_of(n * VT, VT), VT), :])
            before = prev_v[n]
            for half in range(2):
                total = tile[half * 128 : half * 128 + 128, :]
                total = total + v_split[before, half, 0:128, :].astype(F32)
                total = total + v_split[before, half, 128:256, :].astype(F32)
                high, low = split(total)
                v_split[n, half, 0:128, :] = high
                v_split[n, half, 128:256, :] = low

    def particle(dst):
        @pl.loop(0, section)
        def _(c):
            slab = window[pl.ds(pl.multiple_of(c * VT, VT), SPAN * VT), :]
            for half in range(2):
                tiles = []
                for o in range(SPAN):
                    tiles.append(v_split[last_v[c * SPAN + o], half])
                product = jnp.dot(
                    jnp.concatenate(tiles, axis=1), slab, preferred_element_type=F32
                )
                both = product[:, 0:128] + product[:, 128:256]
                to = pl.ds(pl.multiple_of(c * VT + half * 128, 128), 128)
                dst[to, :] = both[0:128, :] + both[128:256, :]

    wait_edges(0, start_a, "recv")
    put_halo(0)
    particle(part_a.at[0])
    send_blocks(1, part_a.at[0], part_b.at[0])
    part_b[0, own, :] = part_a[0, own, :]

    w_load.wait()

    @pl.loop(0, wslots)
    def _(n):
        tile = jnp.transpose(w_stage[pl.ds(pl.multiple_of(n * OT, OT), OT), :])
        high, low = split(tile)
        for k in range(2):
            at = pl.ds(pl.multiple_of(n * 2 * OT + k * OT, OT), OT)
            w_split[at, 0:128] = high
            w_split[at, 128:256] = low

    my_virt = virt_rows[pl.ds(lax.div(me * block, 128), 1), :] if block < 128 else None
    if block < 128:
        virt_wide[pl.ds(0, 128), :] = wide(my_virt)
        first = pl.multiple_of(lax.rem(me * block, 128), block)
    else:
        for j in range(block // 128):
            virt_wide[pl.ds(j * 128, 128), :] = wide(
                virt_rows[pl.ds(me * (block // 128) + j, 1), :]
            )
        first = 0

    def put_split(q, values):
        high, low = split(values)
        split_b[q, :, 0:128] = high
        split_b[q, :, 128:256] = low

    def hole(dst):
        @pl.loop(0, wslots)
        def _(n):
            weight = w_split[pl.ds(pl.multiple_of(n * 2 * OT, 2 * OT), 2 * OT), :]
            product = jnp.dot(split_b[w_cols[n]], weight, preferred_element_type=F32)
            chain[n] = product[:, 0:128] + product[:, 128:256] + chain[prev_w[n]]

        @pl.loop(0, count)
        def _(r):
            dst[blk(r), :] = chain[last_w[r]]

    pltpu.make_async_remote_copy(
        src_ref=occ_all.at[pl.ds(0, count - 1)],
        dst_ref=occ_all.at[pl.ds(0, count - 1)],
        send_sem=occ_sem.at[0],
        recv_sem=occ_sem.at[1],
        device_id={"pair": others[0]},
        device_id_type=MESH,
    ).wait_recv()
    wait_blocks(0, start_a, start_b, "recv")

    @pl.loop(0, count)
    def _(q):
        at = blk(q)
        row = occ_all[pl.ds(q, 1)].reshape(1, 128)
        scale_b[at, :] = 1.0 / (virt_wide[pl.ds(first, block), :] + row)
        put_split(q, start_b[at, :])

    hole(hole_b.at[0])
    send_blocks(2, hole_b.at[0], hole_a.at[0])
    hole_a[0, own, :] = hole_b[0, own, :]

    def advance_b(k):
        @pl.loop(0, count)
        def _(q):
            at = blk(q)
            put_split(q, start_b[at, :] + (part_b[k, at, :] + hole_b[k, at, :]) * scale_b[at, :])

    def advance_a(k):
        for i in list(range(REACH)) + list(range(section - REACH, section)):
            at = pl.ds(i * VT, VT)
            edge[k, at, :] = (
                start_a[at, :] + (part_a[k, at, :] + hole_a[k, at, :]) * scale_a[at, :]
            )
        send_edges(k + 1, edge.at[k])
        for i in list(range(REACH)) + list(range(section - REACH, section)):
            put_window(pl.ds((i + REACH) * VT, VT), edge[k, pl.ds(i * VT, VT), :])

        @pl.loop(REACH, section - REACH)
        def _(i):
            at = pl.ds(pl.multiple_of(i * VT, VT), VT)
            put_window(
                pl.ds(pl.multiple_of((i + REACH) * VT, VT), VT),
                start_a[at, :] + (part_a[k, at, :] + hole_a[k, at, :]) * scale_a[at, :],
            )

        wait_edges(k + 1, edge.at[k], "recv")
        put_halo(k + 1)

    wait_blocks(1, part_a.at[0], part_b.at[0], "recv")
    advance_b(0)
    hole(hole_b.at[1])
    send_blocks(3, hole_b.at[1], hole_a.at[1])
    hole_a[1, own, :] = hole_b[1, own, :]

    wait_blocks(2, hole_b.at[0], hole_a.at[0], "recv")
    advance_a(0)
    particle(part_a.at[1])
    send_blocks(4, part_a.at[1], part_b.at[1])
    part_b[1, own, :] = part_a[1, own, :]

    wait_blocks(3, hole_b.at[1], hole_a.at[1], "recv")
    advance_a(1)
    particle(part_a.at[2])

    wait_blocks(4, part_a.at[1], part_b.at[1], "recv")
    advance_b(1)
    hole(hole_b.at[2])
    send_blocks(5, hole_b.at[2], hole_a.at[2])
    hole_a[2, own, :] = hole_b[2, own, :]

    wait_blocks(5, hole_b.at[2], hole_a.at[2], "recv")

    @pl.loop(0, section)
    def _(i):
        at = pl.ds(pl.multiple_of(i * VT, VT), VT)
        s_buf[at, :] = start_a[at, :] + (part_a[2, at, :] + hole_a[2, at, :]) * scale_a[at, :]

    store = pltpu.make_async_copy(s_buf, out, load_sem.at[0])
    store.start()
    pltpu.make_async_remote_copy(
        src_ref=occ_all.at[pl.ds(0, count - 1)],
        dst_ref=occ_all.at[pl.ds(0, count - 1)],
        send_sem=occ_sem.at[0],
        recv_sem=occ_sem.at[1],
        device_id={"pair": others[0]},
        device_id_type=MESH,
    ).wait_send()
    wait_blocks(0, start_a, start_b, "send")
    wait_blocks(1, part_a.at[0], part_b.at[0], "send")
    wait_blocks(2, hole_b.at[0], hole_a.at[0], "send")
    wait_blocks(3, hole_b.at[1], hole_a.at[1], "send")
    wait_blocks(4, part_a.at[1], part_b.at[1], "send")
    wait_blocks(5, hole_b.at[2], hole_a.at[2], "send")
    wait_edges(0, start_a, "send")
    wait_edges(1, edge.at[0], "send")
    wait_edges(2, edge.at[1], "send")
    store.wait()


def local(
    count,
    sections,
    source,
    occ_energy,
    virt_energy,
    v_tiles,
    v_rows,
    v_cols,
    v_count,
    w_tiles,
    w_rows,
    w_cols,
):
    rows = source.shape[0]
    block = rows // count
    section = rows // VT
    slots, wslots = v_tiles.shape[0], w_tiles.shape[0]
    lists = tables(v_rows, v_cols, v_count, w_rows, section, count)
    smem = pl.BlockSpec(memory_space=pltpu.SMEM)
    hbm = pl.BlockSpec(memory_space=pl.ANY)
    vmem = pltpu.VMEM
    dma = pltpu.SemaphoreType.DMA
    whole = vmem((rows, 128), F32)
    return pl.pallas_call(
        functools.partial(kernel, count, sections),
        out_shape=jax.ShapeDtypeStruct((rows, 128), F32),
        in_specs=[smem] * 5 + [hbm] * 5,
        out_specs=hbm,
        scratch_shapes=[
            whole,
            vmem((1, 128), F32),
            vmem((count, 1, 128), F32),
            vmem((rows // 128, 128), F32),
            vmem((max(block, 128), 128), F32),
            vmem((slots * VT, VT), F32),
            vmem((wslots * OT, OT), F32),
            vmem((slots + 1, 2, VT, VT), BF16),
            vmem((wslots * 2 * OT, 2 * OT), BF16),
            whole,
            whole,
            whole,
            whole,
            vmem((3, rows, 128), F32),
            vmem((2, rows, 128), F32),
            vmem((3, rows, 128), F32),
            vmem((3, rows, 128), F32),
            vmem(((section + 2 * REACH) * VT, 256), BF16),
            vmem((count, block, 256), BF16),
            vmem((wslots + 1, block, 128), F32),
            vmem((2, rows, 128), F32),
            vmem((3, 2 * REACH * VT, 128), F32),
            dma((4,)),
            dma((4,)),
            dma((2,)),
            dma((6,)),
            dma((6,)),
            dma((3, 2)),
            dma((3, 2)),
        ],
        compiler_params=pltpu.CompilerParams(
            collective_id=0, has_side_effects=True, vmem_limit_bytes=62 * 1024 * 1024
        ),
        name="ladders",
    )(
        *lists,
        w_cols,
        source,
        occ_energy.reshape(1, 128),
        virt_energy.reshape(rows // 128, 128),
        v_tiles.reshape(slots * VT, VT),
        w_tiles.reshape(wslots * OT, OT),
    )


def solution(mesh):
    in_specs = (
        P("sec", "pair"),
        P("pair"),
        P("sec"),
        P("sec", None, None),
        P("sec"),
        P("sec"),
        P("sec"),
        P(),
        P(),
        P(),
    )
    body = functools.partial(local, mesh.shape["pair"], mesh.shape["sec"])
    return jax.shard_map(
        body, mesh=mesh, in_specs=in_specs, out_specs=P("sec", "pair"), check_vma=False
    )
```

```python
import functools

import jax
import jax.numpy as jnp
from jax import lax
from jax.experimental import pallas as pl
from jax.experimental.pallas import tpu as pltpu
from jax.sharding import PartitionSpec as P

MESH = pl.DeviceIdType.MESH
VT = 256
OT = 128
REACH = 2
SPAN = 2 * REACH + 1
F32 = jnp.float32
BF16 = jnp.bfloat16
UNROLL = 8
VMEM_LIMIT = 62 * 1024 * 1024


def split(x):
    high = x.astype(BF16)
    low = (x - high.astype(F32)).astype(BF16)
    return high, low


def last_match(keys, queries, depth, earlier):
    column = jnp.transpose(jnp.broadcast_to(keys, (128, 128)))[0:depth, :]
    n = lax.broadcasted_iota(jnp.int32, (depth, 128), 0)
    match = column == queries
    if earlier:
        match = match & (n < lax.broadcasted_iota(jnp.int32, (depth, 128), 1))
    found = jnp.max(jnp.where(match, n, -1), axis=0, keepdims=True)
    return jnp.where(found < 0, depth, found)


def far_first():
    steps = [(dx, dy, dc) for dx in range(-1, 3) for dy in range(-1, 3) for dc in range(2)]
    steps.remove((0, 0, 0))
    return sorted(steps, key=lambda s: -abs(s[0]) - abs(s[1]))


def partners(me, count):
    if count != 32:
        return [lax.rem(me + k, count) for k in range(1, count)]
    y, x, c = lax.div(me, 8), lax.rem(lax.div(me, 2), 4), lax.rem(me, 2)
    return [
        lax.rem(y + dy + 4, 4) * 8 + lax.rem(x + dx + 4, 4) * 2 + lax.rem(c + dc, 2)
        for dx, dy, dc in far_first()
    ]


def kernel(
    count,
    sections,
    v_count,
    w_cols,
    v_rows,
    v_cols,
    w_rows,
    source,
    occ,
    virt,
    v_tiles,
    w_tiles,
    out,
    s_buf,
    occ_own,
    occ_all,
    virt_rows,
    virt_wide,
    v_row,
    v_col,
    w_row,
    keys,
    table,
    index,
    v_stage,
    w_stage,
    v_split,
    w_split,
    start_a,
    scale_a,
    start_b,
    scale_b,
    part_a,
    part_b,
    hole_b,
    hole_a,
    window,
    split_b,
    chain,
    edge,
    halo,
    load_sem,
    list_sem,
    v_sem,
    occ_sem,
    send_sem,
    recv_sem,
    edge_sem,
    halo_sem,
    store_sem,
):
    rows = source.shape[0]
    block = rows // count
    half = block // 2
    section = rows // VT
    slots = v_tiles.shape[0] // VT
    wslots = w_tiles.shape[0] // OT
    groups = v_sem.shape[0]
    per_group = slots // groups
    me = lax.axis_index("pair")
    z = lax.axis_index("sec")
    up, down = lax.rem(z + 1, sections), lax.rem(z + sections - 1, sections)

    loads = [
        pltpu.make_async_copy(occ, occ_own, load_sem.at[1]),
        pltpu.make_async_copy(virt, virt_rows, load_sem.at[2]),
        pltpu.make_async_copy(source, s_buf, load_sem.at[0]),
    ]
    for copy in loads:
        copy.start()
    list_loads = [
        pltpu.make_async_copy(v_rows, v_row, list_sem.at[0]),
        pltpu.make_async_copy(v_cols, v_col, list_sem.at[1]),
        pltpu.make_async_copy(w_rows, w_row, list_sem.at[2]),
    ]
    for copy in list_loads:
        copy.start()
    v_loads = []
    for g in range(groups):
        part = pl.ds(g * per_group * VT, per_group * VT)
        v_loads.append(pltpu.make_async_copy(v_tiles.at[part], v_stage.at[part], v_sem.at[g]))
        v_loads[-1].start()
    w_load = pltpu.make_async_copy(w_tiles, w_stage, load_sem.at[3])
    w_load.start()

    barrier = pltpu.get_barrier_semaphore()

    @pl.loop(1, count)
    def _(k):
        pl.semaphore_signal(
            barrier, inc=1, device_id={"pair": lax.rem(me + k, count)}, device_id_type=MESH
        )

    pl.semaphore_signal(barrier, inc=1, device_id={"sec": up}, device_id_type=MESH)
    pl.semaphore_signal(barrier, inc=1, device_id={"sec": down}, device_id_type=MESH)

    def blk(d):
        return pl.ds(pl.multiple_of(d * block, block), block)

    def piece(d, part, parts):
        size = block // parts
        return pl.ds(pl.multiple_of(d * block + part * size, size), size)

    own = blk(me)
    others = partners(me, count)

    for copy in loads:
        copy.wait()

    def wide(row):
        return jnp.transpose(jnp.broadcast_to(row, (128, 128)))

    @pl.loop(0, rows // 128, unroll=4)
    def _(j):
        at = pl.ds(pl.multiple_of(j * 128, 128), 128)
        scale = 1.0 / (wide(virt_rows[pl.ds(j, 1), :]) + occ_own[...])
        scale_a[at, :] = scale
        start_a[at, :] = s_buf[at, :] * scale

    pl.semaphore_wait(barrier, count - 1 + 2)

    edge_rows = REACH * VT

    def edge_copies(k, ref):
        return [
            pltpu.make_async_remote_copy(
                src_ref=ref.at[pl.ds(first, edge_rows)],
                dst_ref=halo.at[k, pl.ds((1 - side) * edge_rows, edge_rows)],
                send_sem=edge_sem.at[k, side],
                recv_sem=halo_sem.at[k, side],
                device_id={"sec": where},
                device_id_type=MESH,
            )
            for side, (first, where) in enumerate(((0, down), (rows - edge_rows, up)))
        ]

    def send_edges(k, ref):
        for copy in edge_copies(k, ref):
            copy.start()

    def wait_edges(k, ref):
        for copy in edge_copies(k, ref):
            copy.wait_recv()

    def send_blocks(phase, src, dst, part=0, parts=1):
        for d in others:
            pltpu.make_async_remote_copy(
                src_ref=src.at[piece(d, part, parts)],
                dst_ref=dst.at[piece(me, part, parts)],
                send_sem=send_sem.at[phase],
                recv_sem=recv_sem.at[phase],
                device_id={"pair": d},
                device_id_type=MESH,
            ).start()

    def all_blocks(phase, src, dst, parts=1):
        all_but_one = pl.ds(0, (rows - block) // parts)
        return pltpu.make_async_remote_copy(
            src_ref=src.at[all_but_one],
            dst_ref=dst.at[all_but_one],
            send_sem=send_sem.at[phase],
            recv_sem=recv_sem.at[phase],
            device_id={"pair": others[0]},
            device_id_type=MESH,
        )

    all_occ = pltpu.make_async_remote_copy(
        src_ref=occ_all.at[pl.ds(0, count - 1)],
        dst_ref=occ_all.at[pl.ds(0, count - 1)],
        send_sem=occ_sem.at[0],
        recv_sem=occ_sem.at[1],
        device_id={"pair": others[0]},
        device_id_type=MESH,
    )

    send_edges(0, start_a)
    send_blocks(0, start_a, start_b)
    for d in others:
        pltpu.make_async_remote_copy(
            src_ref=occ_own,
            dst_ref=occ_all.at[me],
            send_sem=occ_sem.at[0],
            recv_sem=occ_sem.at[1],
            device_id={"pair": d},
            device_id_type=MESH,
        ).start()
    occ_all[pl.ds(me, 1)] = occ_own[...].reshape(1, 1, 128)
    start_b[own, :] = start_a[own, :]

    for copy in list_loads:
        copy.wait()
    lane = lax.broadcasted_iota(jnp.int32, (1, 128), 1)
    keys[...] = jnp.full((2, 128), -1, jnp.int32)
    listed = v_col[...] * SPAN + v_row[...] - v_col[...]
    keys[0:1, 0:slots] = jnp.where(lane[:, 0:slots] < v_count[0], listed, -1)
    keys[1:2, 0:wslots] = w_row[...]
    v_key, w_key = keys[0:1, :], keys[1:2, :]
    table[0:1, :] = last_match(v_key, lane, slots, False)
    table[1:2, :] = last_match(v_key, v_key, slots, True)
    table[2:3, :] = last_match(w_key, lane, wslots, False)
    table[3:4, :] = last_match(w_key, w_key, wslots, True)
    to_index = pltpu.make_async_copy(table, index, list_sem.at[3])
    to_index.start()

    def put_window(at, values):
        high, low = split(values)
        window[at, 0:128] = high
        window[at, 128:256] = low

    def put_halo(k):
        for i in range(2 * REACH):
            first = i * VT if i < REACH else (section + i) * VT
            put_window(pl.ds(first, VT), halo[k, pl.ds(i * VT, VT), :])

    @pl.loop(0, section)
    def _(i):
        put_window(
            pl.ds(pl.multiple_of((i + REACH) * VT, VT), VT),
            start_a[pl.ds(pl.multiple_of(i * VT, VT), VT), :],
        )

    v_split[slots] = jnp.zeros((2 * VT, VT), BF16)
    chain[wslots] = jnp.zeros((block, OT), F32)
    to_index.wait()

    for g in range(groups):
        v_loads[g].wait()

        @pl.loop(g * per_group, (g + 1) * per_group)
        def _(n):
            tile = jnp.transpose(v_stage[pl.ds(pl.multiple_of(n * VT, VT), VT), :])
            before = index[1, n]
            total = tile + v_split[before, 0:VT, :].astype(F32)
            total = total + v_split[before, VT : 2 * VT, :].astype(F32)
            high, low = split(total)
            v_split[n, 0:VT, :] = high
            v_split[n, VT : 2 * VT, :] = low

    def particle(dst, first, last):
        @pl.loop(first, last)
        def _(c):
            slab = window[pl.ds(pl.multiple_of(c * VT, VT), SPAN * VT), :]
            tiles = [v_split[index[0, c * SPAN + o]] for o in range(SPAN)]
            product = jnp.dot(jnp.concatenate(tiles, axis=1), slab, preferred_element_type=F32)
            both = product[:, 0:128] + product[:, 128:256]
            dst[pl.ds(pl.multiple_of(c * VT, VT), VT), :] = both[0:VT, :] + both[VT : 2 * VT, :]

    def particle_ends(k, ref, dst):
        wait_edges(k, ref)
        put_halo(k)
        particle(dst, 0, REACH)
        particle(dst, section - REACH, section)

    w_load.wait()

    @pl.loop(0, wslots, unroll=2)
    def _(n):
        tile = jnp.transpose(w_stage[pl.ds(pl.multiple_of(n * OT, OT), OT), :])
        high, low = split(tile)
        w_split[n, :, 0:128] = high
        w_split[n, :, 128:256] = low

    particle(part_a.at[0], REACH, section - REACH)
    particle_ends(0, start_a, part_a.at[0])
    send_blocks(1, part_a.at[0], part_b.at[0])
    part_b[0, own, :] = part_a[0, own, :]

    per_row = max(block // 128, 1)
    for j in range(per_row):
        row = lax.div(me * block, 128) + j
        virt_wide[pl.ds(j * 128, 128), :] = wide(virt_rows[pl.ds(row, 1), :])
    first = pl.multiple_of(lax.rem(me * block, 128), block) if block < 128 else 0

    def put_split(q, values, part):
        high, low = split(values)
        split_b[part, q, 0:half, :] = high
        split_b[part, q, half:block, :] = low

    def hole(dst, parts):
        size = len(parts) * half
        to = pl.ds(parts[0] * half, size)

        @pl.loop(0, wslots, step=UNROLL)
        def _(n0):
            sums = []
            for k in range(UNROLL):
                n = n0 + k
                at = w_cols[n]
                left = [split_b[part, at] for part in parts]
                left = left[0] if len(left) == 1 else jnp.concatenate(left, axis=0)
                product = jnp.dot(left, w_split[n], preferred_element_type=F32)
                both = product[:, 0:128] + product[:, 128:256]
                both = [
                    both[i * block : i * block + half] + both[i * block + half : (i + 1) * block]
                    for i in range(len(parts))
                ]
                sums.append(both[0] if len(both) == 1 else jnp.concatenate(both, axis=0))
            for k in range(UNROLL):
                chain[n0 + k, to, :] = sums[k] + chain[index[3, n0 + k], to, :]

        @pl.loop(0, count, unroll=4)
        def _(r):
            at = pl.ds(pl.multiple_of(r * block + parts[0] * half, half), size)
            dst[at, :] = chain[index[2, r], to, :]

    all_occ.wait_recv()

    @pl.loop(0, count, unroll=4)
    def _(q):
        row = occ_all[pl.ds(q, 1)].reshape(1, 128)
        scale_b[blk(q), :] = 1.0 / (virt_wide[pl.ds(first, block), :] + row)

    all_blocks(0, start_a, start_b).wait_recv()

    @pl.loop(0, count, unroll=4)
    def _(q):
        for part in range(2):
            put_split(q, start_b[piece(q, part, 2), :], part)

    hole(hole_b.at[0], (0, 1))
    send_blocks(2, hole_b.at[0], hole_a.at[0])
    hole_a[0, own, :] = hole_b[0, own, :]

    def advance_b(k, parts):
        @pl.loop(0, count, unroll=4)
        def _(q):
            for part in parts:
                at = piece(q, part, 2)
                change = (part_b[k, at, :] + hole_b[k, at, :]) * scale_b[at, :]
                put_split(q, start_b[at, :] + change, part)

    ends = list(range(REACH)) + list(range(section - REACH, section))

    def advance_a(k):
        def moved(at):
            return start_a[at, :] + (part_a[k, at, :] + hole_a[k, at, :]) * scale_a[at, :]

        for i in ends:
            at = pl.ds(i * VT, VT)
            edge[k, at, :] = moved(at)
        send_edges(k + 1, edge.at[k])
        for i in ends:
            put_window(pl.ds((i + REACH) * VT, VT), edge[k, pl.ds(i * VT, VT), :])

        @pl.loop(REACH, section - REACH)
        def _(i):
            at = pl.ds(pl.multiple_of(i * VT, VT), VT)
            put_window(pl.ds(pl.multiple_of((i + REACH) * VT, VT), VT), moved(at))

        particle(part_a.at[k + 1], REACH, section - REACH)
        particle_ends(k + 1, edge.at[k], part_a.at[k + 1])

    all_blocks(1, part_a.at[0], part_b.at[0]).wait_recv()
    advance_b(0, (0, 1))
    hole(hole_b.at[1], (0, 1))
    send_blocks(3, hole_b.at[1], hole_a.at[1])
    hole_a[1, own, :] = hole_b[1, own, :]

    all_blocks(2, hole_b.at[0], hole_a.at[0]).wait_recv()
    advance_a(0)
    for part in range(2):
        send_blocks(4 + part, part_a.at[1], part_b.at[1], part, 2)
    part_b[1, own, :] = part_a[1, own, :]

    all_blocks(3, hole_b.at[1], hole_a.at[1]).wait_recv()
    advance_a(1)

    for part in range(2):
        all_blocks(4 + part, part_a.at[1], part_b.at[1], 2).wait_recv()
        advance_b(1, (part,))
        hole(hole_b.at[2], (part,))
        send_blocks(6 + part, hole_b.at[2], hole_a.at[2], part, 2)
    hole_a[2, own, :] = hole_b[2, own, :]

    @pl.loop(0, section)
    def _(i):
        at = pl.ds(pl.multiple_of(i * VT, VT), VT)
        s_buf[at, :] = start_a[at, :] + part_a[2, at, :] * scale_a[at, :]

    for part in range(2):
        all_blocks(6 + part, hole_b.at[2], hole_a.at[2], 2).wait_recv()
    stores = []
    for i in range(section):
        at = pl.ds(i * VT, VT)
        s_buf[at, :] = s_buf[at, :] + hole_a[2, at, :] * scale_a[at, :]
        stores.append(pltpu.make_async_copy(s_buf.at[at], out.at[at], store_sem.at[i]))
        stores[-1].start()

    all_occ.wait_send()
    all_blocks(0, start_a, start_b).wait_send()
    all_blocks(1, part_a.at[0], part_b.at[0]).wait_send()
    all_blocks(2, hole_b.at[0], hole_a.at[0]).wait_send()
    all_blocks(3, hole_b.at[1], hole_a.at[1]).wait_send()
    for part in range(2):
        all_blocks(4 + part, part_a.at[1], part_b.at[1], 2).wait_send()
        all_blocks(6 + part, hole_b.at[2], hole_a.at[2], 2).wait_send()
    for k, ref in enumerate((start_a, edge.at[0], edge.at[1])):
        for copy in edge_copies(k, ref):
            copy.wait_send()
    for copy in stores:
        copy.wait()


def local(
    count,
    sections,
    source,
    occ_energy,
    virt_energy,
    v_tiles,
    v_rows,
    v_cols,
    v_count,
    w_tiles,
    w_rows,
    w_cols,
):
    rows = source.shape[0]
    block = rows // count
    section = rows // VT
    slots, wslots = v_tiles.shape[0], w_tiles.shape[0]
    smem = pl.BlockSpec(memory_space=pltpu.SMEM)
    hbm = pl.BlockSpec(memory_space=pl.ANY)
    vmem = pltpu.VMEM
    dma = pltpu.SemaphoreType.DMA
    whole = vmem((rows, 128), F32)
    return pl.pallas_call(
        functools.partial(kernel, count, sections),
        out_shape=jax.ShapeDtypeStruct((rows, 128), F32),
        in_specs=[smem] * 2 + [hbm] * 8,
        out_specs=hbm,
        scratch_shapes=[
            whole,
            vmem((1, 128), F32),
            vmem((count, 1, 128), F32),
            vmem((rows // 128, 128), F32),
            vmem((max(block, 128), 128), F32),
            vmem((1, slots), jnp.int32),
            vmem((1, slots), jnp.int32),
            vmem((1, wslots), jnp.int32),
            vmem((2, 128), jnp.int32),
            vmem((8, 128), jnp.int32),
            pltpu.SMEM((8, 128), jnp.int32),
            vmem((slots * VT, VT), F32),
            vmem((wslots * OT, OT), F32),
            vmem((slots + 1, 2 * VT, VT), BF16),
            vmem((wslots, OT, 2 * OT), BF16),
            whole,
            whole,
            whole,
            whole,
            vmem((3, rows, 128), F32),
            vmem((2, rows, 128), F32),
            vmem((3, rows, 128), F32),
            vmem((3, rows, 128), F32),
            vmem(((section + 2 * REACH) * VT, 256), BF16),
            vmem((2, count, block, 128), BF16),
            vmem((wslots + 1, block, 128), F32),
            vmem((2, rows, 128), F32),
            vmem((3, 2 * REACH * VT, 128), F32),
            dma((4,)),
            dma((4,)),
            dma((4,)),
            dma((2,)),
            dma((8,)),
            dma((8,)),
            dma((3, 2)),
            dma((3, 2)),
            dma((section,)),
        ],
        compiler_params=pltpu.CompilerParams(
            collective_id=0, has_side_effects=True, vmem_limit_bytes=VMEM_LIMIT
        ),
        name="ladders",
    )(
        v_count,
        w_cols,
        v_rows.reshape(1, slots),
        v_cols.reshape(1, slots),
        w_rows.reshape(1, wslots),
        source,
        occ_energy.reshape(1, 128),
        virt_energy.reshape(rows // 128, 128),
        v_tiles.reshape(slots * VT, VT),
        w_tiles.reshape(wslots * OT, OT),
    )


def solution(mesh):
    in_specs = (
        P("sec", "pair"),
        P("pair"),
        P("sec"),
        P("sec", None, None),
        P("sec"),
        P("sec"),
        P("sec"),
        P(),
        P(),
        P(),
    )
    body = functools.partial(local, mesh.shape["pair"], mesh.shape["sec"])
    return jax.shard_map(
        body, mesh=mesh, in_specs=in_specs, out_specs=P("sec", "pair"), check_vma=False
    )
```

```python
import functools

import jax
import jax.numpy as jnp
from jax import lax
from jax.experimental import pallas as pl
from jax.experimental.pallas import tpu as pltpu
from jax.sharding import PartitionSpec as P

MESH = pl.DeviceIdType.MESH
VT = 256
OT = 128
REACH = 2
SPAN = 2 * REACH + 1
F32 = jnp.float32
BF16 = jnp.bfloat16
UNROLL = 8
VMEM_LIMIT = 52 * 1024 * 1024


def split(x):
    high = x.astype(BF16)
    low = (x - high.astype(F32)).astype(BF16)
    return high, low


def last_match(keys, queries, depth, earlier):
    column = jnp.transpose(jnp.broadcast_to(keys, (128, 128)))[0:depth, :]
    n = lax.broadcasted_iota(jnp.int32, (depth, 128), 0)
    match = column == queries
    if earlier:
        match = match & (n < lax.broadcasted_iota(jnp.int32, (depth, 128), 1))
    found = jnp.max(jnp.where(match, n, -1), axis=0, keepdims=True)
    return jnp.where(found < 0, depth, found)


def far_first():
    steps = [(dx, dy, dc) for dx in range(-1, 3) for dy in range(-1, 3) for dc in range(2)]
    steps.remove((0, 0, 0))
    return sorted(steps, key=lambda s: -abs(s[0]) - abs(s[1]))


def partners(me, count):
    if count != 32:
        return [lax.rem(me + k, count) for k in range(1, count)]
    y, x, c = lax.div(me, 8), lax.rem(lax.div(me, 2), 4), lax.rem(me, 2)
    return [
        lax.rem(y + dy + 4, 4) * 8 + lax.rem(x + dx + 4, 4) * 2 + lax.rem(c + dc, 2)
        for dx, dy, dc in far_first()
    ]


def kernel(
    count,
    sections,
    v_count,
    w_cols,
    v_rows,
    v_cols,
    w_rows,
    source,
    occ,
    virt,
    v_tiles,
    w_tiles,
    out,
    s_buf,
    occ_own,
    occ_all,
    virt_rows,
    virt_wide,
    virt_b,
    v_row,
    v_col,
    w_row,
    keys,
    table,
    index,
    v_stage,
    w_stage,
    v_split,
    w_split,
    start_a,
    scale_a,
    start_b,
    scale_b,
    part_a,
    part_b,
    hole_b,
    hole_a,
    window,
    split_b,
    chain,
    edge,
    halo,
    load_sem,
    list_sem,
    v_sem,
    occ_sem,
    send_sem,
    recv_sem,
    edge_sem,
    halo_sem,
):
    section = source.shape[0]
    strip = VT // count
    block = section * strip
    half = block // 2
    slots_half = section // 2
    slots = v_tiles.shape[0] // VT
    wslots = w_tiles.shape[0] // OT
    groups = v_sem.shape[0]
    per_group = slots // groups
    me = lax.axis_index("pair")
    z = lax.axis_index("sec")
    up, down = lax.rem(z + 1, sections), lax.rem(z + sections - 1, sections)

    barrier = pltpu.get_barrier_semaphore()

    @pl.loop(1, count)
    def _(k):
        pl.semaphore_signal(
            barrier, inc=1, device_id={"pair": lax.rem(me + k, count)}, device_id_type=MESH
        )

    pl.semaphore_signal(barrier, inc=1, device_id={"sec": up}, device_id_type=MESH)
    pl.semaphore_signal(barrier, inc=1, device_id={"sec": down}, device_id_type=MESH)

    loads = [
        pltpu.make_async_copy(occ, occ_own, load_sem.at[1]),
        pltpu.make_async_copy(virt, virt_rows, load_sem.at[2]),
        pltpu.make_async_copy(source, s_buf, load_sem.at[0]),
    ]
    for copy in loads:
        copy.start()
    list_loads = [
        pltpu.make_async_copy(v_rows, v_row, list_sem.at[0]),
        pltpu.make_async_copy(v_cols, v_col, list_sem.at[1]),
        pltpu.make_async_copy(w_rows, w_row, list_sem.at[2]),
    ]
    for copy in list_loads:
        copy.start()
    v_loads = []
    for g in range(groups):
        part = pl.ds(g * per_group * VT, per_group * VT)
        v_loads.append(pltpu.make_async_copy(v_tiles.at[part], v_stage.at[part], v_sem.at[g]))
        v_loads[-1].start()
    w_load = pltpu.make_async_copy(w_tiles, w_stage, load_sem.at[3])
    w_load.start()

    inner = [(REACH, 0, section - 2 * REACH)]
    outer = [(0, slots_half, REACH), (section - REACH, slots_half + REACH, REACH)]
    spans = (inner, outer)
    tile_of_slot = [t + i for span in spans for t, _, n in span for i in range(n)]

    def strips(d):
        return pl.ds(pl.multiple_of(d * strip, strip), strip)

    def piece(q, part):
        return pl.ds(q * section + part * slots_half, slots_half)

    others = partners(me, count)

    def send(phase, part, src, dst, back):
        for d in others:
            for tile, slot, n in spans[part]:
                if back:
                    from_ = src.at[pl.ds(d * section + slot, n)]
                    to = dst.at[pl.ds(tile, n), strips(me)]
                else:
                    from_ = src.at[pl.ds(tile, n), strips(d)]
                    to = dst.at[pl.ds(me * section + slot, n)]
                pltpu.make_async_remote_copy(
                    src_ref=from_,
                    dst_ref=to,
                    send_sem=send_sem.at[phase, part],
                    recv_sem=recv_sem.at[phase, part],
                    device_id={"pair": d},
                    device_id_type=MESH,
                ).start()

    def keep(src, dst, back):
        for slot, tile in enumerate(tile_of_slot):
            if back:
                dst[tile, strips(me), :] = src[me * section + slot]
            else:
                dst[me * section + slot] = src[tile, strips(me), :]

    def all_of(phase, part, dst):
        some = dst.at[pl.ds(0, (count - 1) * slots_half)]
        return pltpu.make_async_remote_copy(
            src_ref=some,
            dst_ref=some,
            send_sem=send_sem.at[phase, part],
            recv_sem=recv_sem.at[phase, part],
            device_id={"pair": others[0]},
            device_id_type=MESH,
        )

    def as_strips(ref):
        return ref.reshape(count * section, strip, 128)

    all_occ = pltpu.make_async_remote_copy(
        src_ref=occ_all.at[pl.ds(0, count - 1)],
        dst_ref=occ_all.at[pl.ds(0, count - 1)],
        send_sem=occ_sem.at[0],
        recv_sem=occ_sem.at[1],
        device_id={"pair": others[0]},
        device_id_type=MESH,
    )

    pl.semaphore_wait(barrier, count - 1 + 2)
    for part in range(2):
        send(0, part, source, start_b, False)
    for d in others:
        pltpu.make_async_remote_copy(
            src_ref=occ,
            dst_ref=occ_all.at[me],
            send_sem=occ_sem.at[0],
            recv_sem=occ_sem.at[1],
            device_id={"pair": d},
            device_id_type=MESH,
        ).start()

    for copy in loads:
        copy.wait()

    def wide(row):
        return jnp.transpose(jnp.broadcast_to(row, (128, 128)))

    @pl.loop(0, section, unroll=2)
    def _(i):
        for j in range(VT // 128):
            at = pl.ds(j * 128, 128)
            virt_row = virt_rows[pl.ds(i * (VT // 128) + j, 1), :]
            scale = 1.0 / (wide(virt_row) + occ_own[...])
            scale_a[i, at, :] = scale
            start_a[i, at, :] = s_buf[i, at, :] * scale

    def edge_copies(k, ref):
        return [
            pltpu.make_async_remote_copy(
                src_ref=ref.at[pl.ds(first, REACH)],
                dst_ref=halo.at[k, pl.ds((1 - side) * REACH, REACH)],
                send_sem=edge_sem.at[k, side],
                recv_sem=halo_sem.at[k, side],
                device_id={"sec": where},
                device_id_type=MESH,
            )
            for side, (first, where) in enumerate(((0, down), (section - REACH, up)))
        ]

    def send_edges(k, ref):
        for copy in edge_copies(k, ref):
            copy.start()

    def wait_edges(k, ref):
        for copy in edge_copies(k, ref):
            copy.wait_recv()

    send_edges(0, start_a)
    occ_all[pl.ds(me, 1)] = occ_own[...].reshape(1, 1, 128)
    keep(s_buf, start_b, False)

    for copy in list_loads:
        copy.wait()
    lane = lax.broadcasted_iota(jnp.int32, (1, 128), 1)
    keys[...] = jnp.full((2, 128), -1, jnp.int32)
    listed = v_col[...] * SPAN + v_row[...] - v_col[...]
    keys[0:1, 0:slots] = jnp.where(lane[:, 0:slots] < v_count[0], listed, -1)
    keys[1:2, 0:wslots] = w_row[...]
    v_key, w_key = keys[0:1, :], keys[1:2, :]
    table[0:1, :] = last_match(v_key, lane, slots, False)
    table[1:2, :] = last_match(v_key, v_key, slots, True)
    table[2:3, :] = last_match(w_key, lane, wslots, False)
    table[3:4, :] = last_match(w_key, w_key, wslots, True)
    to_index = pltpu.make_async_copy(table, index, list_sem.at[3])
    to_index.start()

    def put_window(i, values):
        high, low = split(values)
        at = pl.ds(pl.multiple_of(i * VT, VT), VT)
        window[at, 0:128] = high
        window[at, 128:256] = low

    def put_halo(k):
        for i in range(2 * REACH):
            put_window(i if i < REACH else section + i, halo[k, i])

    @pl.loop(0, section)
    def _(i):
        put_window(i + REACH, start_a[i])

    v_split[slots] = jnp.zeros((2 * VT, VT), BF16)
    chain[wslots] = jnp.zeros((block, OT), F32)
    to_index.wait()

    for g in range(groups):
        v_loads[g].wait()

        @pl.loop(g * per_group, (g + 1) * per_group)
        def _(n):
            tile = jnp.transpose(v_stage[pl.ds(pl.multiple_of(n * VT, VT), VT), :])
            before = index[1, n]
            total = tile + v_split[before, 0:VT, :].astype(F32)
            total = total + v_split[before, VT : 2 * VT, :].astype(F32)
            high, low = split(total)
            v_split[n, 0:VT, :] = high
            v_split[n, VT : 2 * VT, :] = low

    def particle(dst, first, last):
        @pl.loop(first, last)
        def _(c):
            slab = window[pl.ds(pl.multiple_of(c * VT, VT), SPAN * VT), :]
            tiles = [v_split[index[0, c * SPAN + o]] for o in range(SPAN)]
            product = jnp.dot(jnp.concatenate(tiles, axis=1), slab, preferred_element_type=F32)
            both = product[:, 0:128] + product[:, 128:256]
            dst[c] = both[0:VT, :] + both[VT : 2 * VT, :]

    def particle_ends(k, ref, dst):
        wait_edges(k, ref)
        put_halo(k)
        particle(dst, 0, REACH)
        particle(dst, section - REACH, section)

    particle(part_a.at[0], REACH, section - REACH)
    send(1, 0, part_a.at[0], part_b.at[0], False)
    particle_ends(0, start_a, part_a.at[0])
    send(1, 1, part_a.at[0], part_b.at[0], False)
    keep(part_a.at[0], part_b.at[0], False)

    w_load.wait()

    @pl.loop(0, wslots, unroll=2)
    def _(n):
        tile = jnp.transpose(w_stage[pl.ds(pl.multiple_of(n * OT, OT), OT), :])
        high, low = split(tile)
        w_split[n, :, 0:128] = high
        w_split[n, :, 128:256] = low

    for slot, tile in enumerate(tile_of_slot):
        row = tile * (VT // 128) + lax.div(me * strip, 128)
        virt_wide[...] = wide(virt_rows[pl.ds(row, 1), :])
        first = pl.multiple_of(lax.rem(me * strip, 128), strip)
        virt_b[slot] = virt_wide[pl.ds(first, strip), :]

    def put_split(q, values, part):
        high, low = split(values)
        split_b[part, q, 0:half, :] = high
        split_b[part, q, half:block, :] = low

    def hole(dst, parts):
        size = len(parts) * half
        to = pl.ds(parts[0] * half, size)

        @pl.loop(0, wslots, step=UNROLL)
        def _(n0):
            sums = []
            for k in range(UNROLL):
                n = n0 + k
                at = w_cols[n]
                left = [split_b[part, at] for part in parts]
                left = left[0] if len(left) == 1 else jnp.concatenate(left, axis=0)
                product = jnp.dot(left, w_split[n], preferred_element_type=F32)
                both = product[:, 0:128] + product[:, 128:256]
                both = [
                    both[i * block : i * block + half] + both[i * block + half : (i + 1) * block]
                    for i in range(len(parts))
                ]
                sums.append(both[0] if len(both) == 1 else jnp.concatenate(both, axis=0))
            for k in range(UNROLL):
                chain[n0 + k, to, :] = sums[k] + chain[index[3, n0 + k], to, :]

        @pl.loop(0, count, unroll=4)
        def _(r):
            at = pl.ds(r * section + parts[0] * slots_half, len(parts) * slots_half)
            dst[at] = chain[index[2, r], to, :].reshape(len(parts) * slots_half, strip, 128)

    all_occ.wait_recv()

    @pl.loop(0, count, unroll=4)
    def _(q):
        row = occ_all[pl.ds(q, 1)].reshape(1, 1, 128)
        scale_b[pl.ds(q * section, section)] = 1.0 / (virt_b[...] + row)

    for part in range(2):
        all_of(0, part, start_b).wait_recv()

    @pl.loop(0, count, unroll=4)
    def _(q):
        for part in range(2):
            at = piece(q, part)
            start = start_b[at] * scale_b[at]
            start_b[at] = start
            put_split(q, start.reshape(half, 128), part)

    hole(hole_b.at[0], (0, 1))
    for part in (1, 0):
        send(2, part, hole_b.at[0], hole_a.at[0], True)
    keep(hole_b.at[0], hole_a.at[0], True)

    def advance_b(k, parts):
        @pl.loop(0, count, unroll=4)
        def _(q):
            for part in parts:
                at = piece(q, part)
                change = (part_b[k, at] + hole_b[k, at]) * scale_b[at]
                put_split(q, (start_b[at] + change).reshape(half, 128), part)

    ends = list(range(REACH)) + list(range(section - REACH, section))

    def advance_a(k, phase):
        def moved(i):
            return start_a[i] + (part_a[k, i] + hole_a[k, i]) * scale_a[i]

        all_of(phase, 1, as_strips(hole_a.at[k])).wait_recv()
        for i in ends:
            edge[k, i] = moved(i)
        send_edges(k + 1, edge.at[k])
        for i in ends:
            put_window(i + REACH, edge[k, i])
        all_of(phase, 0, as_strips(hole_a.at[k])).wait_recv()

        @pl.loop(REACH, section - REACH)
        def _(i):
            put_window(i + REACH, moved(i))

        particle(part_a.at[k + 1], REACH, section - REACH)

    for part in range(2):
        all_of(1, part, part_b.at[0]).wait_recv()
        advance_b(0, (part,))
    hole(hole_b.at[1], (0, 1))
    for part in (1, 0):
        send(3, part, hole_b.at[1], hole_a.at[1], True)
    keep(hole_b.at[1], hole_a.at[1], True)

    advance_a(0, 2)
    send(4, 0, part_a.at[1], part_b.at[1], False)
    particle_ends(1, edge.at[0], part_a.at[1])
    send(4, 1, part_a.at[1], part_b.at[1], False)
    keep(part_a.at[1], part_b.at[1], False)

    advance_a(1, 3)

    for part in range(2):
        all_of(4, part, part_b.at[1]).wait_recv()
        advance_b(1, (part,))
        hole(hole_b.at[2], (part,))
        send(5, part, hole_b.at[2], hole_a.at[2], True)
    keep(hole_b.at[2], hole_a.at[2], True)
    particle_ends(2, edge.at[1], part_a.at[2])

    @pl.loop(0, section)
    def _(i):
        s_buf[i] = start_a[i] + part_a[2, i] * scale_a[i]

    for part in range(2):
        all_of(5, part, as_strips(hole_a.at[2])).wait_recv()
        for tile, _, n in spans[part]:

            @pl.loop(tile, tile + n)
            def _(i):
                out[i] = s_buf[i] + hole_a[2, i] * scale_a[i]

    all_occ.wait_send()
    for phase in range(6):
        for part in range(2):
            all_of(phase, part, start_b).wait_send()
    for k, ref in enumerate((start_a, edge.at[0], edge.at[1])):
        for copy in edge_copies(k, ref):
            copy.wait_send()


def local(
    count,
    sections,
    source,
    occ_energy,
    virt_energy,
    v_tiles,
    v_rows,
    v_cols,
    v_count,
    w_tiles,
    w_rows,
    w_cols,
):
    rows = source.shape[0]
    block = rows // count
    section = rows // VT
    strip = VT // count
    slots, wslots = v_tiles.shape[0], w_tiles.shape[0]
    smem = pl.BlockSpec(memory_space=pltpu.SMEM)
    hbm = pl.BlockSpec(memory_space=pl.ANY)
    vmem = pltpu.VMEM
    dma = pltpu.SemaphoreType.DMA
    whole = vmem((section, VT, 128), F32)
    turned = vmem((count * section, strip, 128), F32)
    return pl.pallas_call(
        functools.partial(kernel, count, sections),
        out_shape=jax.ShapeDtypeStruct((section, VT, 128), F32),
        in_specs=[smem] * 2 + [hbm] * 8,
        out_specs=pl.BlockSpec(memory_space=pltpu.VMEM),
        scratch_shapes=[
            whole,
            vmem((1, 128), F32),
            vmem((count, 1, 128), F32),
            vmem((rows // 128, 128), F32),
            vmem((128, 128), F32),
            vmem((section, strip, 128), F32),
            vmem((1, slots), jnp.int32),
            vmem((1, slots), jnp.int32),
            vmem((1, wslots), jnp.int32),
            vmem((2, 128), jnp.int32),
            vmem((8, 128), jnp.int32),
            pltpu.SMEM((8, 128), jnp.int32),
            vmem((slots * VT, VT), F32),
            vmem((wslots * OT, OT), F32),
            vmem((slots + 1, 2 * VT, VT), BF16),
            vmem((wslots, OT, 2 * OT), BF16),
            whole,
            whole,
            turned,
            turned,
            vmem((3, section, VT, 128), F32),
            vmem((2, count * section, strip, 128), F32),
            vmem((3, count * section, strip, 128), F32),
            vmem((3, section, VT, 128), F32),
            vmem(((section + 2 * REACH) * VT, 256), BF16),
            vmem((2, count, block, 128), BF16),
            vmem((wslots + 1, block, 128), F32),
            vmem((2, section, VT, 128), F32),
            vmem((3, 2 * REACH, VT, 128), F32),
            dma((4,)),
            dma((4,)),
            dma((4,)),
            dma((2,)),
            dma((6, 2)),
            dma((6, 2)),
            dma((3, 2)),
            dma((3, 2)),
        ],
        compiler_params=pltpu.CompilerParams(
            collective_id=0, has_side_effects=True, vmem_limit_bytes=VMEM_LIMIT
        ),
        name="ladders",
    )(
        v_count,
        w_cols,
        v_rows.reshape(1, slots),
        v_cols.reshape(1, slots),
        w_rows.reshape(1, wslots),
        source.reshape(section, VT, 128),
        occ_energy.reshape(1, 128),
        virt_energy.reshape(rows // 128, 128),
        v_tiles.reshape(slots * VT, VT),
        w_tiles.reshape(wslots * OT, OT),
    ).reshape(rows, 128)


def solution(mesh):
    in_specs = (
        P("sec", "pair"),
        P("pair"),
        P("sec"),
        P("sec", None, None),
        P("sec"),
        P("sec"),
        P("sec"),
        P(),
        P(),
        P(),
    )
    body = functools.partial(local, mesh.shape["pair"], mesh.shape["sec"])
    return jax.shard_map(
        body, mesh=mesh, in_specs=in_specs, out_specs=P("sec", "pair"), check_vma=False
    )
```

```python
import functools

import jax
import jax.numpy as jnp
from jax import lax
from jax.experimental import pallas as pl
from jax.experimental.pallas import tpu as pltpu
from jax.sharding import PartitionSpec as P

MESH = pl.DeviceIdType.MESH
VT = 256
OT = 128
REACH = 2
SPAN = 2 * REACH + 1
F32 = jnp.float32
BF16 = jnp.bfloat16
UNROLL = 8
VMEM_LIMIT = 62 * 1024 * 1024


def split(x):
    high = x.astype(BF16)
    low = (x - high.astype(F32)).astype(BF16)
    return high, low


def last_match(keys, queries, depth, earlier):
    column = jnp.transpose(jnp.broadcast_to(keys, (128, 128)))[0:depth, :]
    n = lax.broadcasted_iota(jnp.int32, (depth, 128), 0)
    match = column == queries
    if earlier:
        match = match & (n < lax.broadcasted_iota(jnp.int32, (depth, 128), 1))
    found = jnp.max(jnp.where(match, n, -1), axis=0, keepdims=True)
    return jnp.where(found < 0, depth, found)


def far_first():
    steps = [(dx, dy, dc) for dx in range(-1, 3) for dy in range(-1, 3) for dc in range(2)]
    steps.remove((0, 0, 0))
    return sorted(steps, key=lambda s: -abs(s[0]) - abs(s[1]))


def partners(me, count):
    if count != 32:
        return [lax.rem(me + k, count) for k in range(1, count)]
    y, x, c = lax.div(me, 8), lax.rem(lax.div(me, 2), 4), lax.rem(me, 2)
    return [
        lax.rem(y + dy + 4, 4) * 8 + lax.rem(x + dx + 4, 4) * 2 + lax.rem(c + dc, 2)
        for dx, dy, dc in far_first()
    ]


def kernel(
    count,
    sections,
    v_count,
    v_rows,
    v_cols,
    w_rows,
    w_cols,
    source,
    occ,
    virt,
    v_tiles,
    w_tiles,
    out,
    s_buf,
    occ_own,
    occ_all,
    virt_rows,
    virt_wide,
    virt_b,
    v_row,
    v_col,
    w_row,
    w_col,
    keys,
    table,
    index,
    v_stage,
    w_stage,
    v_split,
    w_split,
    start_a,
    scale_a,
    start_b,
    scale_b,
    part_a,
    part_b,
    hole_b,
    hole_a,
    window,
    split_b,
    chain,
    edge,
    halo,
    load_sem,
    list_sem,
    v_sem,
    occ_sem,
    send_sem,
    recv_sem,
    edge_sem,
    halo_sem,
    store_sem,
):
    section = source.shape[0]
    strip = VT // count
    block = section * strip
    half = block // 2
    slots_half = section // 2
    slots = v_tiles.shape[0] // VT
    wslots = w_tiles.shape[0] // OT
    groups = v_sem.shape[0]
    per_group = slots // groups
    me = lax.axis_index("pair")
    z = lax.axis_index("sec")
    up, down = lax.rem(z + 1, sections), lax.rem(z + sections - 1, sections)

    barrier = pltpu.get_barrier_semaphore()

    @pl.loop(1, count)
    def _(k):
        pl.semaphore_signal(
            barrier, inc=1, device_id={"pair": lax.rem(me + k, count)}, device_id_type=MESH
        )

    pl.semaphore_signal(barrier, inc=1, device_id={"sec": up}, device_id_type=MESH)
    pl.semaphore_signal(barrier, inc=1, device_id={"sec": down}, device_id_type=MESH)

    loads = [
        pltpu.make_async_copy(occ, occ_own, load_sem.at[1]),
        pltpu.make_async_copy(virt, virt_rows, load_sem.at[2]),
        pltpu.make_async_copy(source, s_buf, load_sem.at[0]),
    ]
    for copy in loads:
        copy.start()
    list_loads = [
        pltpu.make_async_copy(v_rows, v_row, list_sem.at[0]),
        pltpu.make_async_copy(v_cols, v_col, list_sem.at[1]),
        pltpu.make_async_copy(w_rows, w_row, list_sem.at[2]),
        pltpu.make_async_copy(w_cols, w_col, list_sem.at[4]),
    ]
    for copy in list_loads:
        copy.start()
    v_loads = []
    for g in range(groups):
        part = pl.ds(g * per_group * VT, per_group * VT)
        v_loads.append(pltpu.make_async_copy(v_tiles.at[part], v_stage.at[part], v_sem.at[g]))
        v_loads[-1].start()
    w_load = pltpu.make_async_copy(w_tiles, w_stage, load_sem.at[3])
    w_load.start()

    inner = [(REACH, 0, section - 2 * REACH)]
    outer = [(0, slots_half, REACH), (section - REACH, slots_half + REACH, REACH)]
    spans = (inner, outer)
    tile_of_slot = [t + i for span in spans for t, _, n in span for i in range(n)]

    def strips(d):
        return pl.ds(pl.multiple_of(d * strip, strip), strip)

    def piece(q, part):
        return pl.ds(q * section + part * slots_half, slots_half)

    others = partners(me, count)

    def send(phase, part, src, dst, back):
        for d in others:
            for tile, slot, n in spans[part]:
                if back:
                    from_ = src.at[pl.ds(d * section + slot, n)]
                    to = dst.at[pl.ds(tile, n), strips(me)]
                else:
                    from_ = src.at[pl.ds(tile, n), strips(d)]
                    to = dst.at[pl.ds(me * section + slot, n)]
                pltpu.make_async_remote_copy(
                    src_ref=from_,
                    dst_ref=to,
                    send_sem=send_sem.at[phase, part],
                    recv_sem=recv_sem.at[phase, part],
                    device_id={"pair": d},
                    device_id_type=MESH,
                ).start()

    def keep(src, dst, back):
        for slot, tile in enumerate(tile_of_slot):
            if back:
                dst[tile, strips(me), :] = src[me * section + slot]
            else:
                dst[me * section + slot] = src[tile, strips(me), :]

    def all_of(phase, part, dst):
        some = dst.at[pl.ds(0, (count - 1) * slots_half)]
        return pltpu.make_async_remote_copy(
            src_ref=some,
            dst_ref=some,
            send_sem=send_sem.at[phase, part],
            recv_sem=recv_sem.at[phase, part],
            device_id={"pair": others[0]},
            device_id_type=MESH,
        )

    def as_strips(ref):
        return ref.reshape(count * section, strip, 128)

    all_occ = pltpu.make_async_remote_copy(
        src_ref=occ_all.at[pl.ds(0, count - 1)],
        dst_ref=occ_all.at[pl.ds(0, count - 1)],
        send_sem=occ_sem.at[0],
        recv_sem=occ_sem.at[1],
        device_id={"pair": others[0]},
        device_id_type=MESH,
    )

    pl.semaphore_wait(barrier, count - 1 + 2)
    for part in range(2):
        send(0, part, source, start_b, False)
    for d in others:
        pltpu.make_async_remote_copy(
            src_ref=occ,
            dst_ref=occ_all.at[me],
            send_sem=occ_sem.at[0],
            recv_sem=occ_sem.at[1],
            device_id={"pair": d},
            device_id_type=MESH,
        ).start()

    for copy in loads:
        copy.wait()

    def wide(row):
        return jnp.transpose(jnp.broadcast_to(row, (128, 128)))

    @pl.loop(0, section, unroll=2)
    def _(i):
        for j in range(VT // 128):
            at = pl.ds(j * 128, 128)
            virt_row = virt_rows[pl.ds(i * (VT // 128) + j, 1), :]
            scale = 1.0 / (wide(virt_row) + occ_own[...])
            scale_a[i, at, :] = scale
            start_a[i, at, :] = s_buf[i, at, :] * scale

    def edge_copies(k, ref):
        return [
            pltpu.make_async_remote_copy(
                src_ref=ref.at[pl.ds(first, REACH)],
                dst_ref=halo.at[k, pl.ds((1 - side) * REACH, REACH)],
                send_sem=edge_sem.at[k, side],
                recv_sem=halo_sem.at[k, side],
                device_id={"sec": where},
                device_id_type=MESH,
            )
            for side, (first, where) in enumerate(((0, down), (section - REACH, up)))
        ]

    def send_edges(k, ref):
        for copy in edge_copies(k, ref):
            copy.start()

    def wait_edges(k, ref):
        for copy in edge_copies(k, ref):
            copy.wait_recv()

    send_edges(0, start_a)
    occ_all[pl.ds(me, 1)] = occ_own[...].reshape(1, 1, 128)
    keep(s_buf, start_b, False)

    for copy in list_loads:
        copy.wait()
    lane = lax.broadcasted_iota(jnp.int32, (1, 128), 1)
    keys[...] = jnp.full((2, 128), -1, jnp.int32)
    listed = v_col[...] * SPAN + v_row[...] - v_col[...]
    keys[0:1, 0:slots] = jnp.where(lane[:, 0:slots] < v_count[0], listed, -1)
    keys[1:2, 0:wslots] = w_row[...]
    v_key, w_key = keys[0:1, :], keys[1:2, :]
    table[...] = jnp.zeros((8, 128), jnp.int32)
    table[0:1, :] = last_match(v_key, lane, slots, False)
    table[1:2, :] = last_match(v_key, v_key, slots, True)
    table[2:3, :] = last_match(w_key, lane, wslots, False)
    table[3:4, :] = last_match(w_key, w_key, wslots, True)
    table[4:5, 0:wslots] = w_col[...]
    to_index = pltpu.make_async_copy(table, index, list_sem.at[3])
    to_index.start()

    def put_window(i, values):
        high, low = split(values)
        at = pl.ds(pl.multiple_of(i * VT, VT), VT)
        window[at, 0:128] = high
        window[at, 128:256] = low

    def put_halo(k):
        for i in range(2 * REACH):
            put_window(i if i < REACH else section + i, halo[k, i])

    @pl.loop(0, section)
    def _(i):
        put_window(i + REACH, start_a[i])

    v_split[slots] = jnp.zeros((2 * VT, VT), BF16)
    chain[wslots] = jnp.zeros((block, OT), F32)
    to_index.wait()

    for g in range(groups):
        v_loads[g].wait()

        @pl.loop(g * per_group, (g + 1) * per_group)
        def _(n):
            tile = jnp.transpose(v_stage[pl.ds(pl.multiple_of(n * VT, VT), VT), :])
            before = index[1, n]
            total = tile + v_split[before, 0:VT, :].astype(F32)
            total = total + v_split[before, VT : 2 * VT, :].astype(F32)
            high, low = split(total)
            v_split[n, 0:VT, :] = high
            v_split[n, VT : 2 * VT, :] = low

    def particle(dst, first, last):
        @pl.loop(first, last)
        def _(c):
            slab = window[pl.ds(pl.multiple_of(c * VT, VT), SPAN * VT), :]
            tiles = [v_split[index[0, c * SPAN + o]] for o in range(SPAN)]
            product = jnp.dot(jnp.concatenate(tiles, axis=1), slab, preferred_element_type=F32)
            both = product[:, 0:128] + product[:, 128:256]
            dst[c] = both[0:VT, :] + both[VT : 2 * VT, :]

    def particle_ends(k, ref, dst):
        wait_edges(k, ref)
        put_halo(k)
        particle(dst, 0, REACH)
        particle(dst, section - REACH, section)

    particle(part_a.at[0], REACH, section - REACH)
    send(1, 0, part_a.at[0], part_b.at[0], False)
    particle_ends(0, start_a, part_a.at[0])
    send(1, 1, part_a.at[0], part_b.at[0], False)
    keep(part_a.at[0], part_b.at[0], False)

    w_load.wait()

    @pl.loop(0, wslots, unroll=2)
    def _(n):
        tile = jnp.transpose(w_stage[pl.ds(pl.multiple_of(n * OT, OT), OT), :])
        high, low = split(tile)
        w_split[n, :, 0:128] = high
        w_split[n, :, 128:256] = low

    for slot, tile in enumerate(tile_of_slot):
        row = tile * (VT // 128) + lax.div(me * strip, 128)
        virt_wide[...] = wide(virt_rows[pl.ds(row, 1), :])
        first = pl.multiple_of(lax.rem(me * strip, 128), strip)
        virt_b[slot] = virt_wide[pl.ds(first, strip), :]

    def put_split(q, values, part):
        high, low = split(values)
        split_b[part, q, 0:half, :] = high
        split_b[part, q, half:block, :] = low

    def hole(dst, parts):
        size = len(parts) * half
        to = pl.ds(parts[0] * half, size)

        @pl.loop(0, wslots, step=UNROLL)
        def _(n0):
            sums = []
            for k in range(UNROLL):
                n = n0 + k
                at = index[4, n]
                left = [split_b[part, at] for part in parts]
                left = left[0] if len(left) == 1 else jnp.concatenate(left, axis=0)
                product = jnp.dot(left, w_split[n], preferred_element_type=F32)
                both = product[:, 0:128] + product[:, 128:256]
                both = [
                    both[i * block : i * block + half] + both[i * block + half : (i + 1) * block]
                    for i in range(len(parts))
                ]
                sums.append(both[0] if len(both) == 1 else jnp.concatenate(both, axis=0))
            for k in range(UNROLL):
                chain[n0 + k, to, :] = sums[k] + chain[index[3, n0 + k], to, :]

        @pl.loop(0, count, unroll=4)
        def _(r):
            at = pl.ds(r * section + parts[0] * slots_half, len(parts) * slots_half)
            dst[at] = chain[index[2, r], to, :].reshape(len(parts) * slots_half, strip, 128)

    all_occ.wait_recv()

    @pl.loop(0, count, unroll=4)
    def _(q):
        row = occ_all[pl.ds(q, 1)].reshape(1, 1, 128)
        scale_b[pl.ds(q * section, section)] = 1.0 / (virt_b[...] + row)

    for part in range(2):
        all_of(0, part, start_b).wait_recv()

    @pl.loop(0, count, unroll=4)
    def _(q):
        for part in range(2):
            at = piece(q, part)
            start = start_b[at] * scale_b[at]
            start_b[at] = start
            put_split(q, start.reshape(half, 128), part)

    hole(hole_b.at[0], (0, 1))
    for part in (1, 0):
        send(2, part, hole_b.at[0], hole_a.at[0], True)
    keep(hole_b.at[0], hole_a.at[0], True)

    def advance_b(k, parts):
        @pl.loop(0, count, unroll=4)
        def _(q):
            for part in parts:
                at = piece(q, part)
                change = (part_b[k, at] + hole_b[k, at]) * scale_b[at]
                put_split(q, (start_b[at] + change).reshape(half, 128), part)

    ends = list(range(REACH)) + list(range(section - REACH, section))

    def advance_a(k, phase):
        def moved(i):
            return start_a[i] + (part_a[k, i] + hole_a[k, i]) * scale_a[i]

        all_of(phase, 1, as_strips(hole_a.at[k])).wait_recv()
        for i in ends:
            edge[k, i] = moved(i)
        send_edges(k + 1, edge.at[k])
        for i in ends:
            put_window(i + REACH, edge[k, i])
        all_of(phase, 0, as_strips(hole_a.at[k])).wait_recv()

        @pl.loop(REACH, section - REACH)
        def _(i):
            put_window(i + REACH, moved(i))

        particle(part_a.at[k + 1], REACH, section - REACH)

    for part in range(2):
        all_of(1, part, part_b.at[0]).wait_recv()
        advance_b(0, (part,))
    hole(hole_b.at[1], (0, 1))
    for part in (1, 0):
        send(3, part, hole_b.at[1], hole_a.at[1], True)
    keep(hole_b.at[1], hole_a.at[1], True)

    advance_a(0, 2)
    send(4, 0, part_a.at[1], part_b.at[1], False)
    particle_ends(1, edge.at[0], part_a.at[1])
    send(4, 1, part_a.at[1], part_b.at[1], False)
    keep(part_a.at[1], part_b.at[1], False)

    advance_a(1, 3)

    for part in range(2):
        all_of(4, part, part_b.at[1]).wait_recv()
        advance_b(1, (part,))
        hole(hole_b.at[2], (part,))
        send(5, part, hole_b.at[2], hole_a.at[2], True)
    keep(hole_b.at[2], hole_a.at[2], True)
    particle_ends(2, edge.at[1], part_a.at[2])

    @pl.loop(0, section)
    def _(i):
        s_buf[i] = start_a[i] + part_a[2, i] * scale_a[i]

    stores = []
    for part in range(2):
        all_of(5, part, as_strips(hole_a.at[2])).wait_recv()
        for tile, _, n in spans[part]:
            for i in range(tile, tile + n):
                s_buf[i] = s_buf[i] + hole_a[2, i] * scale_a[i]
                stores.append(pltpu.make_async_copy(s_buf.at[i], out.at[i], store_sem.at[i]))
                stores[-1].start()

    all_occ.wait_send()
    for phase in range(6):
        for part in range(2):
            all_of(phase, part, start_b).wait_send()
    for k, ref in enumerate((start_a, edge.at[0], edge.at[1])):
        for copy in edge_copies(k, ref):
            copy.wait_send()
    for copy in stores:
        copy.wait()


def local(
    count,
    sections,
    source,
    occ_energy,
    virt_energy,
    v_tiles,
    v_rows,
    v_cols,
    v_count,
    w_tiles,
    w_rows,
    w_cols,
):
    rows = source.shape[0]
    block = rows // count
    section = rows // VT
    strip = VT // count
    slots, wslots = v_tiles.shape[0], w_tiles.shape[0]
    hbm = pl.BlockSpec(memory_space=pl.ANY)
    vmem = pltpu.VMEM
    dma = pltpu.SemaphoreType.DMA
    whole = vmem((section, VT, 128), F32)
    turned = vmem((count * section, strip, 128), F32)
    return pl.pallas_call(
        functools.partial(kernel, count, sections),
        out_shape=jax.ShapeDtypeStruct((section, VT, 128), F32),
        in_specs=[pl.BlockSpec(memory_space=pltpu.SMEM)] + [hbm] * 9,
        out_specs=hbm,
        scratch_shapes=[
            whole,
            vmem((1, 128), F32),
            vmem((count, 1, 128), F32),
            vmem((rows // 128, 128), F32),
            vmem((128, 128), F32),
            vmem((section, strip, 128), F32),
            vmem((1, slots), jnp.int32),
            vmem((1, slots), jnp.int32),
            vmem((1, wslots), jnp.int32),
            vmem((1, wslots), jnp.int32),
            vmem((2, 128), jnp.int32),
            vmem((8, 128), jnp.int32),
            pltpu.SMEM((8, 128), jnp.int32),
            vmem((slots * VT, VT), F32),
            vmem((wslots * OT, OT), F32),
            vmem((slots + 1, 2 * VT, VT), BF16),
            vmem((wslots, OT, 2 * OT), BF16),
            whole,
            whole,
            turned,
            turned,
            vmem((3, section, VT, 128), F32),
            vmem((2, count * section, strip, 128), F32),
            vmem((3, count * section, strip, 128), F32),
            vmem((3, section, VT, 128), F32),
            vmem(((section + 2 * REACH) * VT, 256), BF16),
            vmem((2, count, block, 128), BF16),
            vmem((wslots + 1, block, 128), F32),
            vmem((2, section, VT, 128), F32),
            vmem((3, 2 * REACH, VT, 128), F32),
            dma((4,)),
            dma((5,)),
            dma((4,)),
            dma((2,)),
            dma((6, 2)),
            dma((6, 2)),
            dma((3, 2)),
            dma((3, 2)),
            dma((section,)),
        ],
        compiler_params=pltpu.CompilerParams(
            collective_id=0, has_side_effects=True, vmem_limit_bytes=VMEM_LIMIT
        ),
        name="ladders",
    )(
        v_count,
        v_rows.reshape(1, slots),
        v_cols.reshape(1, slots),
        w_rows.reshape(1, wslots),
        w_cols.reshape(1, wslots),
        source.reshape(section, VT, 128),
        occ_energy.reshape(1, 128),
        virt_energy.reshape(rows // 128, 128),
        v_tiles.reshape(slots * VT, VT),
        w_tiles.reshape(wslots * OT, OT),
    ).reshape(rows, 128)


def solution(mesh):
    in_specs = (
        P("sec", "pair"),
        P("pair"),
        P("sec"),
        P("sec", None, None),
        P("sec"),
        P("sec"),
        P("sec"),
        P(),
        P(),
        P(),
    )
    body = functools.partial(local, mesh.shape["pair"], mesh.shape["sec"])
    return jax.shard_map(
        body, mesh=mesh, in_specs=in_specs, out_specs=P("sec", "pair"), check_vma=False
    )
```

```python
import functools

import jax
import jax.numpy as jnp
from jax import lax
from jax.experimental import pallas as pl
from jax.experimental.pallas import tpu as pltpu
from jax.sharding import PartitionSpec as P

MESH = pl.DeviceIdType.MESH
VT = 256
OT = 128
REACH = 2
SPAN = 2 * REACH + 1
F32 = jnp.float32
BF16 = jnp.bfloat16
UNROLL = 8
VMEM_LIMIT = 62 * 1024 * 1024


def split(x):
    high = x.astype(BF16)
    low = (x - high.astype(F32)).astype(BF16)
    return high, low


def last_match(keys, queries, depth, earlier):
    column = jnp.transpose(jnp.broadcast_to(keys, (128, 128)))[0:depth, :]
    n = lax.broadcasted_iota(jnp.int32, (depth, 128), 0)
    match = column == queries
    if earlier:
        match = match & (n < lax.broadcasted_iota(jnp.int32, (depth, 128), 1))
    found = jnp.max(jnp.where(match, n, -1), axis=0, keepdims=True)
    return jnp.where(found < 0, depth, found)


def far_first():
    steps = [(dx, dy, dc) for dx in range(-1, 3) for dy in range(-1, 3) for dc in range(2)]
    steps.remove((0, 0, 0))
    return sorted(steps, key=lambda s: -abs(s[0]) - abs(s[1]))


def partners(me, count):
    if count != 32:
        return [lax.rem(me + k, count) for k in range(1, count)]
    y, x, c = lax.div(me, 8), lax.rem(lax.div(me, 2), 4), lax.rem(me, 2)
    return [
        lax.rem(y + dy + 4, 4) * 8 + lax.rem(x + dx + 4, 4) * 2 + lax.rem(c + dc, 2)
        for dx, dy, dc in far_first()
    ]


def kernel(
    count,
    sections,
    v_count,
    v_rows,
    v_cols,
    w_rows,
    w_cols,
    source,
    occ,
    virt,
    v_tiles,
    w_tiles,
    base_out,
    change_out,
    s_buf,
    occ_own,
    occ_all,
    virt_rows,
    virt_wide,
    virt_b,
    v_row,
    v_col,
    w_row,
    w_col,
    keys,
    table,
    index,
    v_stage,
    w_stage,
    v_split,
    w_split,
    start_a,
    scale_a,
    start_b,
    scale_b,
    part_a,
    part_b,
    hole_b,
    hole_a,
    window,
    split_b,
    chain,
    edge,
    halo,
    load_sem,
    list_sem,
    v_sem,
    occ_sem,
    send_sem,
    recv_sem,
    edge_sem,
    halo_sem,
    store_sem,
):
    section = source.shape[0]
    strip = VT // count
    block = section * strip
    half = block // 2
    slots_half = section // 2
    slots = v_tiles.shape[0] // VT
    wslots = w_tiles.shape[0] // OT
    groups = v_sem.shape[0]
    per_group = slots // groups
    me = lax.axis_index("pair")
    z = lax.axis_index("sec")
    up, down = lax.rem(z + 1, sections), lax.rem(z + sections - 1, sections)

    barrier = pltpu.get_barrier_semaphore()

    @pl.loop(1, count)
    def _(k):
        pl.semaphore_signal(
            barrier, inc=1, device_id={"pair": lax.rem(me + k, count)}, device_id_type=MESH
        )

    pl.semaphore_signal(barrier, inc=1, device_id={"sec": up}, device_id_type=MESH)
    pl.semaphore_signal(barrier, inc=1, device_id={"sec": down}, device_id_type=MESH)

    loads = [
        pltpu.make_async_copy(occ, occ_own, load_sem.at[1]),
        pltpu.make_async_copy(virt, virt_rows, load_sem.at[2]),
        pltpu.make_async_copy(source, s_buf, load_sem.at[0]),
    ]
    for copy in loads:
        copy.start()
    list_loads = [
        pltpu.make_async_copy(v_rows, v_row, list_sem.at[0]),
        pltpu.make_async_copy(v_cols, v_col, list_sem.at[1]),
        pltpu.make_async_copy(w_rows, w_row, list_sem.at[2]),
        pltpu.make_async_copy(w_cols, w_col, list_sem.at[4]),
    ]
    for copy in list_loads:
        copy.start()
    v_loads = []
    for g in range(groups):
        part = pl.ds(g * per_group * VT, per_group * VT)
        v_loads.append(pltpu.make_async_copy(v_tiles.at[part], v_stage.at[part], v_sem.at[g]))
        v_loads[-1].start()
    w_load = pltpu.make_async_copy(w_tiles, w_stage, load_sem.at[3])
    w_load.start()

    inner = [(REACH, 0, section - 2 * REACH)]
    outer = [(0, slots_half, REACH), (section - REACH, slots_half + REACH, REACH)]
    spans = (inner, outer)
    tile_of_slot = [t + i for span in spans for t, _, n in span for i in range(n)]

    def strips(d):
        return pl.ds(pl.multiple_of(d * strip, strip), strip)

    def piece(q, part):
        return pl.ds(q * section + part * slots_half, slots_half)

    others = partners(me, count)

    def send(phase, part, src, dst, back):
        for d in others:
            for tile, slot, n in spans[part]:
                if back:
                    from_ = src.at[pl.ds(d * section + slot, n)]
                    to = dst.at[pl.ds(tile, n), strips(me)]
                else:
                    from_ = src.at[pl.ds(tile, n), strips(d)]
                    to = dst.at[pl.ds(me * section + slot, n)]
                pltpu.make_async_remote_copy(
                    src_ref=from_,
                    dst_ref=to,
                    send_sem=send_sem.at[phase, part],
                    recv_sem=recv_sem.at[phase, part],
                    device_id={"pair": d},
                    device_id_type=MESH,
                ).start()

    def keep(src, dst, back):
        for slot, tile in enumerate(tile_of_slot):
            if back:
                dst[tile, strips(me), :] = src[me * section + slot]
            else:
                dst[me * section + slot] = src[tile, strips(me), :]

    def all_of(phase, part, dst):
        some = dst.at[pl.ds(0, (count - 1) * slots_half)]
        return pltpu.make_async_remote_copy(
            src_ref=some,
            dst_ref=some,
            send_sem=send_sem.at[phase, part],
            recv_sem=recv_sem.at[phase, part],
            device_id={"pair": others[0]},
            device_id_type=MESH,
        )

    def as_strips(ref):
        return ref.reshape(count * section, strip, 128)

    all_occ = pltpu.make_async_remote_copy(
        src_ref=occ_all.at[pl.ds(0, count - 1)],
        dst_ref=occ_all.at[pl.ds(0, count - 1)],
        send_sem=occ_sem.at[0],
        recv_sem=occ_sem.at[1],
        device_id={"pair": others[0]},
        device_id_type=MESH,
    )

    pl.semaphore_wait(barrier, count - 1 + 2)
    for part in range(2):
        send(0, part, source, start_b, False)
    for d in others:
        pltpu.make_async_remote_copy(
            src_ref=occ,
            dst_ref=occ_all.at[me],
            send_sem=occ_sem.at[0],
            recv_sem=occ_sem.at[1],
            device_id={"pair": d},
            device_id_type=MESH,
        ).start()

    for copy in loads:
        copy.wait()

    def wide(row):
        return jnp.transpose(jnp.broadcast_to(row, (128, 128)))

    @pl.loop(0, section, unroll=2)
    def _(i):
        for j in range(VT // 128):
            at = pl.ds(j * 128, 128)
            virt_row = virt_rows[pl.ds(i * (VT // 128) + j, 1), :]
            scale = 1.0 / (wide(virt_row) + occ_own[...])
            scale_a[i, at, :] = scale
            start_a[i, at, :] = s_buf[i, at, :] * scale

    def edge_copies(k, ref):
        return [
            pltpu.make_async_remote_copy(
                src_ref=ref.at[pl.ds(first, REACH)],
                dst_ref=halo.at[k, pl.ds((1 - side) * REACH, REACH)],
                send_sem=edge_sem.at[k, side],
                recv_sem=halo_sem.at[k, side],
                device_id={"sec": where},
                device_id_type=MESH,
            )
            for side, (first, where) in enumerate(((0, down), (section - REACH, up)))
        ]

    def send_edges(k, ref):
        for copy in edge_copies(k, ref):
            copy.start()

    def wait_edges(k, ref):
        for copy in edge_copies(k, ref):
            copy.wait_recv()

    send_edges(0, start_a)
    occ_all[pl.ds(me, 1)] = occ_own[...].reshape(1, 1, 128)
    keep(s_buf, start_b, False)

    for copy in list_loads:
        copy.wait()
    lane = lax.broadcasted_iota(jnp.int32, (1, 128), 1)
    keys[...] = jnp.full((2, 128), -1, jnp.int32)
    listed = v_col[...] * SPAN + v_row[...] - v_col[...]
    keys[0:1, 0:slots] = jnp.where(lane[:, 0:slots] < v_count[0], listed, -1)
    keys[1:2, 0:wslots] = w_row[...]
    v_key, w_key = keys[0:1, :], keys[1:2, :]
    table[...] = jnp.zeros((8, 128), jnp.int32)
    table[0:1, :] = last_match(v_key, lane, slots, False)
    table[1:2, :] = last_match(v_key, v_key, slots, True)
    table[2:3, :] = last_match(w_key, lane, wslots, False)
    table[3:4, :] = last_match(w_key, w_key, wslots, True)
    table[4:5, 0:wslots] = w_col[...]
    to_index = pltpu.make_async_copy(table, index, list_sem.at[3])
    to_index.start()

    def put_window(i, values):
        high, low = split(values)
        at = pl.ds(pl.multiple_of(i * VT, VT), VT)
        window[at, 0:128] = high
        window[at, 128:256] = low

    def put_halo(k):
        for i in range(2 * REACH):
            put_window(i if i < REACH else section + i, halo[k, i])

    @pl.loop(0, section)
    def _(i):
        put_window(i + REACH, start_a[i])

    v_split[slots] = jnp.zeros((2 * VT, VT), BF16)
    chain[wslots] = jnp.zeros((block, OT), F32)
    to_index.wait()

    for g in range(groups):
        v_loads[g].wait()

        @pl.loop(g * per_group, (g + 1) * per_group)
        def _(n):
            tile = jnp.transpose(v_stage[pl.ds(pl.multiple_of(n * VT, VT), VT), :])
            before = index[1, n]
            total = tile + v_split[before, 0:VT, :].astype(F32)
            total = total + v_split[before, VT : 2 * VT, :].astype(F32)
            high, low = split(total)
            v_split[n, 0:VT, :] = high
            v_split[n, VT : 2 * VT, :] = low

    def particle(dst, first, last):
        @pl.loop(first, last)
        def _(c):
            slab = window[pl.ds(pl.multiple_of(c * VT, VT), SPAN * VT), :]
            tiles = [v_split[index[0, c * SPAN + o]] for o in range(SPAN)]
            product = jnp.dot(jnp.concatenate(tiles, axis=1), slab, preferred_element_type=F32)
            both = product[:, 0:128] + product[:, 128:256]
            dst[c] = both[0:VT, :] + both[VT : 2 * VT, :]

    def particle_ends(k, ref, dst):
        wait_edges(k, ref)
        put_halo(k)
        particle(dst, 0, REACH)
        particle(dst, section - REACH, section)

    particle(part_a.at[0], REACH, section - REACH)
    send(1, 0, part_a.at[0], part_b.at[0], False)
    particle_ends(0, start_a, part_a.at[0])
    send(1, 1, part_a.at[0], part_b.at[0], False)
    keep(part_a.at[0], part_b.at[0], False)

    w_load.wait()

    @pl.loop(0, wslots, unroll=2)
    def _(n):
        tile = jnp.transpose(w_stage[pl.ds(pl.multiple_of(n * OT, OT), OT), :])
        high, low = split(tile)
        w_split[n, :, 0:128] = high
        w_split[n, :, 128:256] = low

    for slot, tile in enumerate(tile_of_slot):
        row = tile * (VT // 128) + lax.div(me * strip, 128)
        virt_wide[...] = wide(virt_rows[pl.ds(row, 1), :])
        first = pl.multiple_of(lax.rem(me * strip, 128), strip)
        virt_b[slot] = virt_wide[pl.ds(first, strip), :]

    def put_split(q, values, part):
        high, low = split(values)
        split_b[part, q, 0:half, :] = high
        split_b[part, q, half:block, :] = low

    def hole(dst, parts, scaled=False):
        size = len(parts) * half
        to = pl.ds(parts[0] * half, size)

        @pl.loop(0, wslots, step=UNROLL)
        def _(n0):
            sums = []
            for k in range(UNROLL):
                n = n0 + k
                at = index[4, n]
                left = [split_b[part, at] for part in parts]
                left = left[0] if len(left) == 1 else jnp.concatenate(left, axis=0)
                product = jnp.dot(left, w_split[n], preferred_element_type=F32)
                both = product[:, 0:128] + product[:, 128:256]
                both = [
                    both[i * block : i * block + half] + both[i * block + half : (i + 1) * block]
                    for i in range(len(parts))
                ]
                sums.append(both[0] if len(both) == 1 else jnp.concatenate(both, axis=0))
            for k in range(UNROLL):
                chain[n0 + k, to, :] = sums[k] + chain[index[3, n0 + k], to, :]

        @pl.loop(0, count, unroll=4)
        def _(r):
            at = pl.ds(r * section + parts[0] * slots_half, len(parts) * slots_half)
            total = chain[index[2, r], to, :].reshape(len(parts) * slots_half, strip, 128)
            dst[at] = total * scale_b[at] if scaled else total

    all_occ.wait_recv()

    @pl.loop(0, count, unroll=4)
    def _(q):
        row = occ_all[pl.ds(q, 1)].reshape(1, 1, 128)
        scale_b[pl.ds(q * section, section)] = 1.0 / (virt_b[...] + row)

    for part in range(2):
        all_of(0, part, start_b).wait_recv()

    @pl.loop(0, count, unroll=4)
    def _(q):
        for part in range(2):
            at = piece(q, part)
            start = start_b[at] * scale_b[at]
            start_b[at] = start
            put_split(q, start.reshape(half, 128), part)

    hole(hole_b.at[0], (0, 1))
    for part in (1, 0):
        send(2, part, hole_b.at[0], hole_a.at[0], True)
    keep(hole_b.at[0], hole_a.at[0], True)

    def advance_b(k, parts):
        @pl.loop(0, count, unroll=4)
        def _(q):
            for part in parts:
                at = piece(q, part)
                change = (part_b[k, at] + hole_b[k, at]) * scale_b[at]
                put_split(q, (start_b[at] + change).reshape(half, 128), part)

    ends = list(range(REACH)) + list(range(section - REACH, section))

    def advance_a(k, phase):
        def moved(i):
            return start_a[i] + (part_a[k, i] + hole_a[k, i]) * scale_a[i]

        all_of(phase, 1, as_strips(hole_a.at[k])).wait_recv()
        for i in ends:
            edge[k, i] = moved(i)
        send_edges(k + 1, edge.at[k])
        for i in ends:
            put_window(i + REACH, edge[k, i])
        all_of(phase, 0, as_strips(hole_a.at[k])).wait_recv()

        @pl.loop(REACH, section - REACH)
        def _(i):
            put_window(i + REACH, moved(i))

        particle(part_a.at[k + 1], REACH, section - REACH)

    for part in range(2):
        all_of(1, part, part_b.at[0]).wait_recv()
        advance_b(0, (part,))
    hole(hole_b.at[1], (0, 1))
    for part in (1, 0):
        send(3, part, hole_b.at[1], hole_a.at[1], True)
    keep(hole_b.at[1], hole_a.at[1], True)

    advance_a(0, 2)
    send(4, 0, part_a.at[1], part_b.at[1], False)
    particle_ends(1, edge.at[0], part_a.at[1])
    send(4, 1, part_a.at[1], part_b.at[1], False)
    keep(part_a.at[1], part_b.at[1], False)

    advance_a(1, 3)

    for part in range(2):
        all_of(4, part, part_b.at[1]).wait_recv()
        advance_b(1, (part,))
        hole(hole_b.at[2], (part,), True)
        send(5, part, hole_b.at[2], change_out, True)
    stores = []
    for tile, slot, n in inner + outer:
        stores.append(
            pltpu.make_async_copy(
                hole_b.at[2, pl.ds(me * section + slot, n)],
                change_out.at[pl.ds(tile, n), strips(me)],
                store_sem.at[len(stores)],
            )
        )
        stores[-1].start()
    particle_ends(2, edge.at[1], part_a.at[2])

    @pl.loop(0, section)
    def _(i):
        s_buf[i] = start_a[i] + part_a[2, i] * scale_a[i]

    stores.append(pltpu.make_async_copy(s_buf, base_out, store_sem.at[len(stores)]))
    stores[-1].start()
    for part in range(2):
        all_of(5, part, as_strips(change_out)).wait_recv()

    all_occ.wait_send()
    for phase in range(6):
        for part in range(2):
            all_of(phase, part, start_b).wait_send()
    for k, ref in enumerate((start_a, edge.at[0], edge.at[1])):
        for copy in edge_copies(k, ref):
            copy.wait_send()
    for copy in stores:
        copy.wait()


def join_kernel(base, change, out, base_buf, change_buf, out_buf, base_sem, change_sem, out_sem):
    pieces = range(base.shape[0])
    loads = []
    for i in pieces:
        loads.append(pltpu.make_async_copy(base.at[i], base_buf.at[i], base_sem.at[i]))
        loads.append(pltpu.make_async_copy(change.at[i], change_buf.at[i], change_sem.at[i]))
    for copy in loads:
        copy.start()
    stores = [pltpu.make_async_copy(out_buf.at[i], out.at[i], out_sem.at[i]) for i in pieces]
    for i in pieces:
        loads[2 * i].wait()
        loads[2 * i + 1].wait()
        out_buf[i] = base_buf[i] + change_buf[i]
        stores[i].start()
    for copy in stores:
        copy.wait()


def join(base, change):
    hbm = pl.BlockSpec(memory_space=pl.ANY)
    return pl.pallas_call(
        join_kernel,
        out_shape=jax.ShapeDtypeStruct(base.shape, base.dtype),
        in_specs=[hbm] * 2,
        out_specs=hbm,
        scratch_shapes=[pltpu.VMEM(base.shape, base.dtype)] * 3
        + [pltpu.SemaphoreType.DMA((base.shape[0],))] * 3,
        compiler_params=pltpu.CompilerParams(vmem_limit_bytes=VMEM_LIMIT),
        name="join",
    )(base, change)


def local(
    count,
    sections,
    source,
    occ_energy,
    virt_energy,
    v_tiles,
    v_rows,
    v_cols,
    v_count,
    w_tiles,
    w_rows,
    w_cols,
):
    rows = source.shape[0]
    block = rows // count
    section = rows // VT
    strip = VT // count
    slots, wslots = v_tiles.shape[0], w_tiles.shape[0]
    hbm = pl.BlockSpec(memory_space=pl.ANY)
    vmem = pltpu.VMEM
    dma = pltpu.SemaphoreType.DMA
    whole = vmem((section, VT, 128), F32)
    turned = vmem((count * section, strip, 128), F32)
    base, change = pl.pallas_call(
        functools.partial(kernel, count, sections),
        out_shape=(jax.ShapeDtypeStruct((section, VT, 128), F32),) * 2,
        in_specs=[pl.BlockSpec(memory_space=pltpu.SMEM)] + [hbm] * 9,
        out_specs=(hbm, hbm),
        scratch_shapes=[
            whole,
            vmem((1, 128), F32),
            vmem((count, 1, 128), F32),
            vmem((rows // 128, 128), F32),
            vmem((128, 128), F32),
            vmem((section, strip, 128), F32),
            vmem((1, slots), jnp.int32),
            vmem((1, slots), jnp.int32),
            vmem((1, wslots), jnp.int32),
            vmem((1, wslots), jnp.int32),
            vmem((2, 128), jnp.int32),
            vmem((8, 128), jnp.int32),
            pltpu.SMEM((8, 128), jnp.int32),
            vmem((slots * VT, VT), F32),
            vmem((wslots * OT, OT), F32),
            vmem((slots + 1, 2 * VT, VT), BF16),
            vmem((wslots, OT, 2 * OT), BF16),
            whole,
            whole,
            turned,
            turned,
            vmem((3, section, VT, 128), F32),
            vmem((2, count * section, strip, 128), F32),
            vmem((3, count * section, strip, 128), F32),
            vmem((2, section, VT, 128), F32),
            vmem(((section + 2 * REACH) * VT, 256), BF16),
            vmem((2, count, block, 128), BF16),
            vmem((wslots + 1, block, 128), F32),
            vmem((2, section, VT, 128), F32),
            vmem((3, 2 * REACH, VT, 128), F32),
            dma((4,)),
            dma((5,)),
            dma((4,)),
            dma((2,)),
            dma((6, 2)),
            dma((6, 2)),
            dma((3, 2)),
            dma((3, 2)),
            dma((4,)),
        ],
        compiler_params=pltpu.CompilerParams(
            collective_id=0, has_side_effects=True, vmem_limit_bytes=VMEM_LIMIT
        ),
        name="ladders",
    )(
        v_count,
        v_rows.reshape(1, slots),
        v_cols.reshape(1, slots),
        w_rows.reshape(1, wslots),
        w_cols.reshape(1, wslots),
        source.reshape(section, VT, 128),
        occ_energy.reshape(1, 128),
        virt_energy.reshape(rows // 128, 128),
        v_tiles.reshape(slots * VT, VT),
        w_tiles.reshape(wslots * OT, OT),
    )
    return join(base, change).reshape(rows, 128)


def solution(mesh):
    in_specs = (
        P("sec", "pair"),
        P("pair"),
        P("sec"),
        P("sec", None, None),
        P("sec"),
        P("sec"),
        P("sec"),
        P(),
        P(),
        P(),
    )
    body = functools.partial(local, mesh.shape["pair"], mesh.shape["sec"])
    return jax.shard_map(
        body, mesh=mesh, in_specs=in_specs, out_specs=P("sec", "pair"), check_vma=False
    )
```
